512 devices in a mesh: dp: 16 (over z_lo, x), block: 32 (over z_hi, y, core).
Axes of the slice: x: 4, y: 4, z: 16 (z_hi: 4, z_lo: 4; z = z_hi * 4 + z_lo), core: 2. Of those that a mesh axis runs over, the one named last changes fastest.
Arguments:
- positions: float32 [3, 131072], P(None, ('dp', 'block')), may hold values from -4 to 4
- neighbours: int32 [16, 131072], P(None, ('dp', 'block')), may hold values from 0 to 32
- atom_species: int32 [131072], P(('dp', 'block')), may hold values from 0 to 3
- tagged_atom: int32 [4096], P(('dp', 'block')), may hold values from 0 to 31
- observed_in: int32 [4096], P(('dp', 'block')), may hold values from 0 to 3
- targets: float32 [64], replicated, may hold values from -3 to 3
- noise_level: float32 [64], replicated, may hold values from 0.1 to 1
- embed_scale: float32 [4, 128], replicated, may hold values from -4 to 4
- embed_shift: float32 [4, 128], replicated, may hold values from -3 to 3
- first_weight: float32 [128, 256], replicated, may hold values from -1.5 to 1.5
- first_bias: float32 [256], replicated, may hold values from -3 to 3
- middle_weight: float32 [256, 256], replicated, may hold values from -0.375 to 0.375
- middle_bias: float32 [256], replicated, may hold values from -3 to 3
- energy_weight: float32 [4, 256], replicated, may hold values from -0.375 to 0.375
- covariance: float32 [32, 2048, 2048], P('block', 'dp'), as said below
Outputs:
- new_weights: float32 [32, 2048], P('block', 'dp')
- new_covariance: float32 [32, 2048, 2048], P('block', 'dp')
The draws below stay inside these ranges and needn't reach their ends.
Inputs may be any that keep to these rules, and one draw needn't show every extreme that they name: `neighbours`: a value of 32 marks an empty slot; any other value counts an atom of the same structure. `tagged_atom`: counted within the structure. `observed_in`: the observation is counted within the structure's group. `covariance`: every block is symmetric and positive definite.
All inputs are finite; a program needn't handle non-finite values.
Results may differ from the reference program's by a relative error of at most 0.0003.
Values sent between devices are 32-bit elements; how exact they have to be, the bound alone decides.
No kernel may reach another device: no remote copies, remote signals or barrier semaphores. Data moves between devices by JAX's collectives and lax.ppermute only.
A program may use at most 64 MiB of HBM per device.

```python
import math
import jax
import jax.numpy as jnp
import numpy as np
from jax import lax

ORDER = 2048
HID = 256
EMB = 128
SPECIES = 4
NNEI = 16
ATOMS_STR = 32
OBS = 64
OBS_DP = 4
WROWS = 256
STRUCTS = 4096
ATOMS = 131072
N_DP = 16
N_BLOCK = 32


def draw_covariance(key, part):
    first_key = jax.random.fold_in(key, 11)
    second_key = jax.random.fold_in(key, 12)
    entries = jax.random.normal(first_key, (N_BLOCK, ORDER, ORDER), jnp.float32)
    symmetric = (entries + jnp.swapaxes(entries, 1, 2)) * (0.45 / math.sqrt(ORDER))
    diagonal = jax.random.uniform(second_key, (N_BLOCK, ORDER), jnp.float32, 2.0, 3.0)
    return symmetric + diagonal[:, :, None] * jnp.eye(ORDER, dtype=jnp.float32)[None]


def set_ends(array, key, smallest, largest):
    place = [jax.random.randint(jax.random.fold_in(key, axis), (), 0, length) for axis, length in enumerate(array.shape)]
    widest = array.shape.index(max(array.shape))
    neighbour = place[:widest] + [(place[widest] + 1) % array.shape[widest]] + place[widest + 1:]
    return array.at[tuple(place)].set(smallest).at[tuple(neighbour)].set(largest)


def block_scale(key, extent, pieces, low, largest):
    def one(position, parts):
        heights = jax.random.uniform(jax.random.fold_in(jax.random.fold_in(key, 6), position), (parts,), jnp.float32, low / len(pieces), largest / len(pieces))
        return jnp.repeat(jnp.exp(heights), extent[position] // parts).reshape((-1,) + (1,) * (len(extent) - position - 1))

    loudness = one(*pieces[0])
    for cut in pieces[1:]:
        loudness = loudness * one(*cut)
    return loudness


def bell_draw(stream_key, extent, deviation, reach, pieces=(), held_as=jnp.bfloat16):
    values = deviation * jax.random.normal(stream_key, extent, jnp.float32)
    if pieces:
        values = values * block_scale(stream_key, extent, pieces, -0.22, 0.18)
    return jnp.clip(values, -reach, reach).astype(held_as)


def setup_inputs(seed: int = 0) -> dict:
    streams_of = jax.random.split(jax.random.key(seed), 16)
    positions = bell_draw(streams_of[0], (3, ATOMS), 1.0, 4.0, ((1, 512),), jnp.float32)
    neighbours = set_ends(jax.random.randint(streams_of[1], (NNEI, ATOMS), 0, ATOMS_STR + 1), jax.random.fold_in(streams_of[1], 1), 0, ATOMS_STR).astype(jnp.int32)
    atom_species = set_ends(jax.random.randint(streams_of[2], (ATOMS,), 0, SPECIES), jax.random.fold_in(streams_of[2], 1), 0, SPECIES - 1).astype(jnp.int32)
    tagged_atom = set_ends(jax.random.randint(streams_of[3], (STRUCTS,), 0, ATOMS_STR), jax.random.fold_in(streams_of[3], 1), 0, ATOMS_STR - 1).astype(jnp.int32)
    observed_in = set_ends(jax.random.randint(streams_of[4], (STRUCTS,), 0, OBS_DP), jax.random.fold_in(streams_of[4], 1), 0, OBS_DP - 1).astype(jnp.int32)
    targets = bell_draw(streams_of[5], (OBS,), 0.5, 3.0, (), jnp.float32)
    noise_level = jnp.clip(jnp.exp(jax.random.uniform(streams_of[6], (OBS,), jnp.float32, math.log(0.1), math.log(1.0))), 0.1, 1.0)
    embed_scale = bell_draw(streams_of[7], (SPECIES, EMB), 1.0, 4.0, (), jnp.float32)
    embed_shift = bell_draw(streams_of[8], (SPECIES, EMB), 0.5, 3.0, (), jnp.float32)
    first_weight = bell_draw(streams_of[9], (EMB, HID), (EMB // 8) ** -0.5, 1.5, (), jnp.float32)
    first_bias = bell_draw(streams_of[10], (HID,), 0.5, 3.0, (), jnp.float32)
    middle_weight = bell_draw(streams_of[11], (HID, HID), HID ** -0.5, 0.375, (), jnp.float32)
    middle_bias = bell_draw(streams_of[12], (HID,), 0.5, 3.0, (), jnp.float32)
    energy_weight = bell_draw(streams_of[13], (SPECIES, HID), HID ** -0.5, 0.375, (), jnp.float32)
    covariance = draw_covariance(jax.random.fold_in(streams_of[15], 71), 0)
    return dict(positions=positions, neighbours=neighbours, atom_species=atom_species, tagged_atom=tagged_atom, observed_in=observed_in, targets=targets, noise_level=noise_level, embed_scale=embed_scale, embed_shift=embed_shift, first_weight=first_weight, first_bias=first_bias, middle_weight=middle_weight, middle_bias=middle_bias, energy_weight=energy_weight, covariance=covariance)


radial_width = 4.0
forgetting = 0.98
highest = lax.Precision.HIGHEST

def observations(window, positions, neighbours, atom_species, tagged_atom, observed_in, embed_scale, embed_shift, first_weight, first_bias, middle_weight, middle_bias, energy_weight, obs_count, weighting):
    atom_total = positions.shape[1]
    struct_total = tagged_atom.shape[0]
    struct_size = atom_total // struct_total
    species_count = embed_scale.shape[0]
    slot_count = neighbours.shape[0]
    struct_start = jnp.arange(atom_total, dtype=jnp.int32) // struct_size * struct_size
    live_slot = (neighbours < struct_size).astype(jnp.float32)
    neighbour_at = struct_start[None, :] + jnp.minimum(neighbours, struct_size - 1)
    near_species = atom_species[neighbour_at]
    species_range = jnp.arange(species_count, dtype=jnp.int32)
    species_table = (near_species[None, :, :] == species_range[:, None, None]).astype(jnp.float32)
    edge_scale = jnp.einsum('se,ska->eka', embed_scale, species_table, precision=highest)
    edge_shift = jnp.einsum('se,ska->eka', embed_shift, species_table, precision=highest)
    own_species = (atom_species[None, :] == species_range[:, None]).astype(jnp.float32)
    readout = jnp.dot(energy_weight.T, own_species, precision=highest)
    remainder = middle_weight[window.shape[0]:]

    def site_energy(coords, middle):
        displace = coords[:, neighbour_at] - coords[:, None, :]
        distance_sq = lax.optimization_barrier(jnp.sum(displace * displace, axis=0))
        radial = jnp.exp(-distance_sq / radial_width) * live_slot
        embedded = jnp.tanh(radial[None] * edge_scale + edge_shift)
        descriptor = lax.optimization_barrier(jnp.sum(radial[None] * embedded, axis=1)) / slot_count
        first_layer = jnp.tanh(jnp.dot(first_weight.T, descriptor, precision=highest) + first_bias[:, None])
        second_layer = jnp.tanh(jnp.dot(middle.T, first_layer, precision=highest) + middle_bias[:, None])
        return lax.optimization_barrier(jnp.sum(readout * second_layer, axis=0))

    def predict(window_part):
        middle = jnp.concatenate([window_part, remainder], axis=0)
        energies, pullback = jax.vjp(lambda coords: site_energy(coords, middle), positions)
        forces = -pullback(jnp.ones_like(energies))[0]
        per_struct = lax.optimization_barrier(jnp.sum(energies.reshape(struct_total, struct_size), axis=1)) / struct_size
        tag_table = (tagged_atom[:, None] == jnp.arange(struct_size, dtype=jnp.int32)[None, :]).astype(jnp.float32)
        picked = lax.optimization_barrier(jnp.sum(forces.reshape(3, struct_total, struct_size) * tag_table[None], axis=2))
        values = jnp.concatenate([per_struct[None, :], picked], axis=0)
        value_rows = values[np.arange(obs_count) % 4]
        chosen = (observed_in[None, :] == jnp.arange(obs_count, dtype=jnp.int32)[:, None]).astype(jnp.float32)
        return lax.optimization_barrier(jnp.sum(chosen * value_rows, axis=1)) * weighting
    predicted, pullback = jax.vjp(predict, window)
    basis = jnp.eye(obs_count, dtype=predicted.dtype)
    jacobian = lax.map(lambda row: pullback(row)[0], basis)
    return (predicted, jacobian)

def reference(positions, neighbours, atom_species, tagged_atom, observed_in, targets, noise_level, embed_scale, embed_shift, first_weight, first_bias, middle_weight, middle_bias, energy_weight, covariance):
    device_total = N_DP * N_BLOCK
    per_device = positions.shape[1] // device_total
    struct_device = tagged_atom.shape[0] // device_total
    window = middle_weight[:WROWS]
    weighting = OBS / tagged_atom.shape[0]
    coords_all = positions.reshape(3, N_DP, N_BLOCK, per_device).transpose(1, 2, 0, 3)
    lists_all = neighbours.reshape(NNEI, N_DP, N_BLOCK, per_device).transpose(1, 2, 0, 3)
    species_all = atom_species.reshape(N_DP, N_BLOCK, per_device)
    tagged_all = tagged_atom.reshape(N_DP, N_BLOCK, struct_device)
    observed_all = observed_in.reshape(N_DP, N_BLOCK, struct_device)

    def one_group(group_inputs):

        def one_device(carry, device_inputs):
            coords, lists, species, tagged, observed = device_inputs
            predicted, jacobian = observations(window, coords, lists, species, tagged, observed, embed_scale, embed_shift, first_weight, first_bias, middle_weight, middle_bias, energy_weight, OBS_DP, weighting)
            return ((carry[0] + predicted, carry[1] + jacobian), None)
        initial = (jnp.zeros((OBS_DP,), positions.dtype), jnp.zeros((OBS_DP, WROWS, HID), positions.dtype))
        return lax.scan(one_device, initial, group_inputs)[0]
    predicted, jacobian = lax.map(one_group, (coords_all, lists_all, species_all, tagged_all, observed_all))
    predicted = predicted.reshape(OBS)
    jacobian = jacobian.reshape(OBS, N_BLOCK, ORDER)
    product = jnp.einsum('bij,obj->bio', covariance, jacobian, precision=highest)
    gram_sum = jnp.einsum('obi,bip->op', jacobian, product, precision=highest)
    gram_sum = 0.5 * (gram_sum + gram_sum.T) + jnp.diag(noise_level)
    factor = jnp.linalg.cholesky(gram_sum)
    inverse = jax.scipy.linalg.cho_solve((factor, True), jnp.eye(OBS, dtype=gram_sum.dtype))
    gain = jnp.einsum('bio,op->bip', product, inverse, precision=highest)
    innovation = targets - predicted
    new_weights = window.reshape(N_BLOCK, ORDER) + jnp.einsum('bio,o->bi', gain, innovation, precision=highest)
    new_covariance = (covariance - jnp.einsum('bio,bjo->bij', gain, product, precision=highest)) / forgetting
    return (new_weights, new_covariance)
```

```python
import functools

import jax
import jax.numpy as jnp
from jax import lax
from jax.experimental import pallas as pl
from jax.experimental.pallas import tpu as pltpu
from jax.sharding import Mesh
from jax.sharding import PartitionSpec as P

OBS = 64
GROUPS = 16
OBS_DP = 4
STRUCT = 32
LOCAL_STRUCTS = 8
ATOMS = 256
LANES = 128
HID = 256
EMB = 128
SLOTS = 16
ORDER = 2048
ROWS = 128
DP = ("dp_0", "dp_1")
BLOCK = ("block_0", "block_1", "block_2")
DP_BLOCK = ("dp_0", "dp_1", "block_0", "block_1", "block_2")

radial_width = 4.0
forgetting = 0.98
highest = lax.Precision.HIGHEST

VMEM = pl.BlockSpec(memory_space=pltpu.VMEM)
SMEM = pl.BlockSpec(memory_space=pltpu.SMEM)


def contract(lhs, rhs, over):
    return lax.dot_general(
        lhs, rhs, ((over[:1], over[1:]), ((), ())), precision=highest, preferred_element_type=jnp.float32
    )


def along_lanes(row, at):
    return jnp.take_along_axis(
        jnp.broadcast_to(row, at.shape), at, axis=1, mode="promise_in_bounds"
    )


def jacobian_kernel(
    place,
    tagged,
    observed,
    positions,
    neighbours,
    species,
    scale,
    shift,
    first_weight,
    first_bias,
    middle_weight,
    middle_bias,
    energy_weight,
    mine,
    theirs,
    predicted,
    window,
    tables,
    descriptor,
    forward,
    heads,
    jacobian,
    weighting,
):
    core, block, group = place[0], place[1], place[2]
    for kind, table in enumerate((scale, shift)):
        columns = table[:].T
        for s in range(4):
            tables[kind * 4 + s] = jnp.broadcast_to(columns[:, s : s + 1], (EMB, LANES))
    lane = lax.broadcasted_iota(jnp.int32, (SLOTS, LANES), 1)
    for half in range(2):
        lanes = slice(half * LANES, (half + 1) * LANES)
        tag = jnp.zeros((SLOTS, LANES), jnp.int32)
        part = jnp.zeros((SLOTS, LANES), jnp.int32)
        for s in range(4):
            here = lane // STRUCT == s
            tag = jnp.where(here, tagged[half * 4 + s], tag)
            part = jnp.where(here, observed[half * 4 + s], part)
        listed = neighbours[:, lanes]
        within = jnp.minimum(listed, STRUCT - 1)
        at = lane // STRUCT * STRUCT + within
        distance_sq = jnp.zeros((SLOTS, LANES), jnp.float32)
        chosen = jnp.zeros((SLOTS, LANES), jnp.float32)
        for c in range(3):
            row = positions[c : c + 1, lanes]
            displace = along_lanes(row, at) - row
            distance_sq = distance_sq + displace * displace
            chosen = jnp.where(part == c + 1, displace, chosen)
        radial = jnp.exp(-distance_sq / radial_width) * (listed < STRUCT).astype(jnp.float32)
        moved = (within == tag).astype(jnp.float32) - (lane % STRUCT == tag).astype(jnp.float32)
        radial_dot = radial * (-2.0 / radial_width) * chosen * moved
        near = along_lanes(species[:, lanes], at)
        odd = (near & 1) == 1
        upper = near >= 2

        def embed(step, carry, half=half, radial=radial, radial_dot=radial_dot, odd=odd, upper=upper):
            start = pl.multiple_of(step * 16, 16)
            rows = pl.ds(start, 16)
            held = [tables[n, rows, :] for n in range(8)]
            total = jnp.zeros((16, LANES), jnp.float32)
            tangent = jnp.zeros((16, LANES), jnp.float32)
            for k in range(SLOTS):
                r = jnp.broadcast_to(radial[k : k + 1], (16, LANES))
                r_dot = jnp.broadcast_to(radial_dot[k : k + 1], (16, LANES))
                is_odd = jnp.broadcast_to(odd[k : k + 1], (16, LANES))
                is_upper = jnp.broadcast_to(upper[k : k + 1], (16, LANES))
                slope = jnp.where(
                    is_upper,
                    jnp.where(is_odd, held[3], held[2]),
                    jnp.where(is_odd, held[1], held[0]),
                )
                offset = jnp.where(
                    is_upper,
                    jnp.where(is_odd, held[7], held[6]),
                    jnp.where(is_odd, held[5], held[4]),
                )
                steep = r * slope
                bent = jnp.tanh(steep + offset)
                total = total + r * bent
                tangent = tangent + r_dot * (bent + steep * (1.0 - bent * bent))
            descriptor[rows, half * LANES : (half + 1) * LANES] = total / SLOTS
            descriptor[rows, ATOMS + half * LANES : ATOMS + (half + 1) * LANES] = tangent / SLOTS
            return carry

        lax.fori_loop(0, EMB // 16, embed, 0)

    inner = contract(descriptor[:], first_weight[:], (0, 0))
    first = jnp.tanh(inner[:ATOMS] + first_bias[:])
    forward[:ATOMS] = first
    forward[ATOMS:] = (1.0 - first * first) * inner[ATOMS:]
    outer = contract(forward[:], middle_weight[:], (1, 0))
    second = jnp.tanh(outer[:ATOMS] + middle_bias[:])
    bend = 1.0 - second * second
    second_dot = bend * outer[ATOMS:]
    own = lax.broadcasted_iota(jnp.int32, (4, ATOMS), 0) == species[:]
    readout = contract(own.astype(jnp.float32), energy_weight[:], (0, 0))
    slope = readout * bend
    slope_dot = -2.0 * readout * second * second_dot
    energy = readout * second
    force = -(readout * second_dot)
    sums = [jnp.zeros((1, HID), jnp.float32) for _ in range(OBS_DP)]
    for s in range(LOCAL_STRUCTS):
        rows = slice(s * STRUCT, (s + 1) * STRUCT)
        q = observed[s]
        is_energy = q == 0
        direct = jnp.where(is_energy, slope[rows] * (weighting / STRUCT), slope_dot[rows] * -weighting)
        through = slope[rows] * -weighting
        value = jnp.sum(
            jnp.where(is_energy, energy[rows] * (weighting / STRUCT), force[rows] * weighting),
            axis=0,
            keepdims=True,
        )
        for o in range(OBS_DP):
            columns = slice(o * HID, (o + 1) * HID)
            heads[s * STRUCT : (s + 1) * STRUCT, columns] = jnp.where(q == o, direct, 0.0)
            heads[ATOMS + s * STRUCT : ATOMS + (s + 1) * STRUCT, columns] = jnp.where(
                q == o, through, 0.0
            )
            sums[o] = sums[o] + jnp.where(q == o, value, 0.0)
    predicted[:] = jnp.zeros((8, LANES), jnp.float32)
    for o in range(OBS_DP):
        predicted[o : o + 1, :] = sums[o][:, :LANES] + sums[o][:, LANES:]
    jacobian[:] = contract(forward[:], heads[:], (0, 0))
    for y in range(4):
        for z in range(4):
            pair = (z * 8 + y * 2) * 8
            kept = pl.multiple_of(pair + core * 8, 8)
            sent = pl.multiple_of(pair + (1 - core) * 8, 8)
            mine[y, z] = jacobian[pl.ds(kept, 8), :]
            theirs[y, z] = jacobian[pl.ds(sent, 8), :]
    line = middle_weight[pl.ds(block * 8 + group // 2, 1), :]
    window[:] = jnp.where(group % 2 == 0, line[:, :LANES], line[:, LANES:])


def product_kernel(gathered, covariance, predicted, columns, sent):
    for i in range(8):
        for q in range(OBS_DP):
            columns[q * GROUPS : (q + 1) * GROUPS, i * HID : (i + 1) * HID] = gathered[
                :, i, q * HID : (q + 1) * HID
            ]
    product = contract(columns[:], covariance[0], (1, 1))
    for d in range(GROUPS):
        sent[d, :OBS] = product
        sent[d, OBS:] = predicted[:]


def gram_kernel(columns, products, sent):
    gram = jnp.zeros((OBS, OBS), jnp.float32)
    for d in range(GROUPS):
        gram = gram + contract(columns[:, d * ROWS : (d + 1) * ROWS], products[d, :OBS], (1, 1))
    half = OBS // 2
    values = jnp.sum(
        jnp.concatenate([products[:, OBS + q, :] for q in range(OBS_DP)], axis=0),
        axis=1,
        keepdims=True,
    )
    packed = jnp.concatenate(
        [
            gram[:half],
            gram[half:, half:],
            values[:half],
            values[half:],
            jnp.zeros((half, half - 2), jnp.float32),
        ],
        axis=1,
    )
    for k in range(8):
        sent[k] = packed


def summed_kernel(arrived, sent):
    total = arrived[0]
    for k in range(1, 8):
        total = total + arrived[k]
    for k in range(4):
        sent[k] = total


def update_kernel(
    place, arrived, products, covariance, window, targets, noise, new_weights, new_covariance, wide
):
    group = place[2]
    half = OBS // 2
    packed = (arrived[0] + arrived[1]) + (arrived[2] + arrived[3])
    corner = packed[:, half:OBS]
    gram = jnp.concatenate(
        [
            packed[:, :OBS],
            jnp.concatenate([corner.T, packed[:, OBS : OBS + half]], axis=1),
        ],
        axis=0,
    )
    gram = 0.5 * (gram + gram.T)
    observed = jnp.concatenate([packed[:, 96:97], packed[:, 97:98]], axis=0)
    down = lax.broadcasted_iota(jnp.int32, (OBS, OBS), 0)
    across = lax.broadcasted_iota(jnp.int32, (OBS, OBS), 1)
    source = across == down % GROUPS * OBS_DP + down // GROUPS
    noise_here = jnp.sum(jnp.where(source, noise[:], 0.0), axis=1, keepdims=True)
    target_here = jnp.sum(jnp.where(source, targets[:], 0.0), axis=1, keepdims=True)
    identity = (down == across).astype(jnp.float32)
    gram = gram + jnp.where(down == across, noise_here, 0.0)
    work = jnp.concatenate([gram, identity], axis=1)
    below = lax.broadcasted_iota(jnp.int32, (OBS, 1), 0)
    pivots = jnp.ones((OBS, 1), jnp.float32)
    for k in range(OBS):
        row = work[k : k + 1, :]
        pivot = row[:, k : k + 1]
        factor = jnp.where(below > k, work[:, k : k + 1] / pivot, 0.0)
        pivots = jnp.where(below == k, pivot, pivots)
        work = work - factor * row
    root = work[:, OBS:] * lax.rsqrt(pivots)
    for d in range(GROUPS):
        wide[:, d * ROWS : (d + 1) * ROWS] = products[d, :OBS]
    own = products[group, :OBS]
    gain = contract(root, contract(root, own, (1, 0)), (0, 0))
    new_weights[:] = window[:] + jnp.sum(gain * (target_here - observed), axis=0, keepdims=True)
    new_covariance[0] = (covariance[0] - contract(gain, wide[:], (0, 0))) / forgetting


def exchanged(tiles, axes):
    return lax.all_to_all(tiles, axes, split_axis=0, concat_axis=0, tiled=True)


def local(
    positions,
    neighbours,
    atom_species,
    tagged_atom,
    observed_in,
    targets,
    noise_level,
    embed_scale,
    embed_shift,
    first_weight,
    first_bias,
    middle_weight,
    middle_bias,
    energy_weight,
    covariance,
    weighting,
):
    f32 = jnp.float32
    place = jnp.stack(
        [lax.axis_index("block_2"), lax.axis_index(BLOCK), lax.axis_index(DP)]
    ).astype(jnp.int32)
    mine, theirs, predicted, window = pl.pallas_call(
        functools.partial(jacobian_kernel, weighting=weighting),
        out_shape=(
            jax.ShapeDtypeStruct((4, 4, 8, OBS_DP * HID), f32),
            jax.ShapeDtypeStruct((4, 4, 8, OBS_DP * HID), f32),
            jax.ShapeDtypeStruct((8, LANES), f32),
            jax.ShapeDtypeStruct((1, LANES), f32),
        ),
        in_specs=[SMEM, SMEM, SMEM] + [VMEM] * 10,
        out_specs=(VMEM, VMEM, VMEM, VMEM),
        scratch_shapes=[
            pltpu.VMEM((8, EMB, LANES), f32),
            pltpu.VMEM((EMB, 2 * ATOMS), f32),
            pltpu.VMEM((2 * ATOMS, HID), f32),
            pltpu.VMEM((2 * ATOMS, OBS_DP * HID), f32),
            pltpu.VMEM((HID, OBS_DP * HID), f32),
        ],
    )(
        place,
        tagged_atom,
        observed_in,
        positions,
        neighbours,
        atom_species[None],
        embed_scale,
        embed_shift,
        first_weight,
        first_bias[None],
        middle_weight,
        middle_bias[None],
        energy_weight,
    )
    partner = mine + lax.ppermute(theirs, "block_2", [(0, 1), (1, 0)])
    across_y = jnp.sum(exchanged(partner, "block_1"), axis=0)
    across_z = jnp.sum(exchanged(across_y, "block_0"), axis=0)
    gathered = exchanged(jnp.broadcast_to(across_z[None], (GROUPS, 8, OBS_DP * HID)), DP)
    columns, sent = pl.pallas_call(
        product_kernel,
        out_shape=(
            jax.ShapeDtypeStruct((OBS, ORDER), f32),
            jax.ShapeDtypeStruct((GROUPS, OBS + 8, ROWS), f32),
        ),
        in_specs=[VMEM] * 3,
        out_specs=(VMEM, VMEM),
    )(gathered, covariance, predicted)
    products = exchanged(sent, DP)
    grams = pl.pallas_call(
        gram_kernel,
        out_shape=jax.ShapeDtypeStruct((8, OBS // 2, LANES), f32),
        in_specs=[VMEM] * 2,
        out_specs=VMEM,
    )(columns, products)
    near = pl.pallas_call(
        summed_kernel,
        out_shape=jax.ShapeDtypeStruct((4, OBS // 2, LANES), f32),
        in_specs=[VMEM],
        out_specs=VMEM,
    )(exchanged(grams, ("block_1", "block_2")))
    return pl.pallas_call(
        update_kernel,
        out_shape=(
            jax.ShapeDtypeStruct((1, ROWS), f32),
            jax.ShapeDtypeStruct((1, ROWS, ORDER), f32),
        ),
        in_specs=[SMEM] + [VMEM] * 6,
        out_specs=(VMEM, VMEM),
        scratch_shapes=[pltpu.VMEM((OBS, ORDER), f32)],
    )(
        place,
        exchanged(near, "block_0"),
        products,
        covariance,
        window,
        targets[None],
        noise_level[None],
    )


def solution(mesh):
    finer = Mesh(
        mesh.devices.reshape(4, 4, 4, 4, 2), ("dp_0", "dp_1", "block_0", "block_1", "block_2")
    )
    placed = (
        P(None, DP_BLOCK),
        P(None, DP_BLOCK),
        P(DP_BLOCK),
        P(DP_BLOCK),
        P(DP_BLOCK),
        P(),
        P(),
        P(),
        P(),
        P(),
        P(),
        P(),
        P(),
        P(),
        P(BLOCK, DP, None),
    )
    weighting = OBS / (LOCAL_STRUCTS * mesh.devices.size)
    return jax.shard_map(
        functools.partial(local, weighting=weighting),
        mesh=finer,
        in_specs=placed,
        out_specs=(P(BLOCK, DP), P(BLOCK, DP, None)),
        check_vma=False,
    )
```

```python
import functools

import jax
import jax.numpy as jnp
from jax import lax
from jax.experimental import pallas as pl
from jax.experimental.pallas import tpu as pltpu
from jax.sharding import Mesh
from jax.sharding import PartitionSpec as P

OBS = 64
GROUPS = 16
OBS_DP = 4
STRUCT = 32
LOCAL_STRUCTS = 8
ATOMS = 256
LANES = 128
HID = 256
EMB = 128
SLOTS = 16
ORDER = 2048
ROWS = 128
DP = ("dp_0", "dp_1")
BLOCK = ("block_0", "block_1", "block_2")
DP_BLOCK = ("dp_0", "dp_1", "block_0", "block_1", "block_2")

radial_width = 4.0
forgetting = 0.98
highest = lax.Precision.HIGHEST

VMEM = pl.BlockSpec(memory_space=pltpu.VMEM)
SMEM = pl.BlockSpec(memory_space=pltpu.SMEM)
HBM = pl.BlockSpec(memory_space=pltpu.HBM)


def granted(mib):
    return pltpu.CompilerParams(vmem_limit_bytes=mib * 1024 * 1024)


def contract(lhs, rhs, over):
    return lax.dot_general(
        lhs, rhs, ((over[:1], over[1:]), ((), ())), precision=highest, preferred_element_type=jnp.float32
    )


def halves(values):
    upper = values.astype(jnp.bfloat16)
    return upper, (values - upper.astype(jnp.float32)).astype(jnp.bfloat16)


def along_lanes(row, at):
    return jnp.take_along_axis(
        jnp.broadcast_to(row, at.shape), at, axis=1, mode="promise_in_bounds"
    )


def jacobian_kernel(
    place,
    tagged,
    observed,
    positions,
    neighbours,
    species,
    scale,
    shift,
    first_source,
    first_bias,
    middle_source,
    middle_bias,
    energy_weight,
    targets,
    noise,
    mine,
    theirs,
    predicted,
    kept,
    tables,
    descriptor,
    forward,
    features,
    heads,
    jacobian,
    first_weight,
    middle_weight,
    arrivals,
    weighting,
):
    core, block, group = place[0], place[1], place[2]
    first_copy = pltpu.make_async_copy(first_source, first_weight, arrivals.at[0])
    middle_copy = pltpu.make_async_copy(middle_source, middle_weight, arrivals.at[1])
    first_copy.start()
    middle_copy.start()
    for kind, table in enumerate((scale, shift)):
        columns = table[:].T
        for s in range(4):
            tables[kind * 4 + s] = jnp.broadcast_to(columns[:, s : s + 1], (EMB, LANES))
    lane = lax.broadcasted_iota(jnp.int32, (SLOTS, LANES), 1)
    for half in range(2):
        lanes = slice(half * LANES, (half + 1) * LANES)
        tag = jnp.zeros((SLOTS, LANES), jnp.int32)
        part = jnp.zeros((SLOTS, LANES), jnp.int32)
        for s in range(4):
            here = lane // STRUCT == s
            tag = jnp.where(here, tagged[half * 4 + s], tag)
            part = jnp.where(here, observed[half * 4 + s], part)
        listed = neighbours[:, lanes]
        within = jnp.minimum(listed, STRUCT - 1)
        at = lane // STRUCT * STRUCT + within
        distance_sq = jnp.zeros((SLOTS, LANES), jnp.float32)
        chosen = jnp.zeros((SLOTS, LANES), jnp.float32)
        for c in range(3):
            row = positions[c : c + 1, lanes]
            displace = along_lanes(row, at) - row
            distance_sq = distance_sq + displace * displace
            chosen = jnp.where(part == c + 1, displace, chosen)
        radial = jnp.exp(-distance_sq / radial_width) * (listed < STRUCT).astype(jnp.float32)
        moved = (within == tag).astype(jnp.float32) - (lane % STRUCT == tag).astype(jnp.float32)
        radial_dot = radial * (-2.0 / radial_width) * chosen * moved
        near = along_lanes(species[:, lanes], at)
        odd = (near & 1) == 1
        upper = near >= 2

        def embed(step, carry, half=half, radial=radial, radial_dot=radial_dot, odd=odd, upper=upper):
            start = pl.multiple_of(step * 16, 16)
            rows = pl.ds(start, 16)
            held = [tables[n, rows, :] for n in range(8)]
            total = jnp.zeros((16, LANES), jnp.float32)
            tangent = jnp.zeros((16, LANES), jnp.float32)
            for k in range(SLOTS):
                r = jnp.broadcast_to(radial[k : k + 1], (16, LANES))
                r_dot = jnp.broadcast_to(radial_dot[k : k + 1], (16, LANES))
                is_odd = jnp.broadcast_to(odd[k : k + 1], (16, LANES))
                is_upper = jnp.broadcast_to(upper[k : k + 1], (16, LANES))
                slope = jnp.where(
                    is_upper,
                    jnp.where(is_odd, held[3], held[2]),
                    jnp.where(is_odd, held[1], held[0]),
                )
                offset = jnp.where(
                    is_upper,
                    jnp.where(is_odd, held[7], held[6]),
                    jnp.where(is_odd, held[5], held[4]),
                )
                steep = r * slope
                bent = jnp.tanh(steep + offset)
                total = total + r * bent
                tangent = tangent + r_dot * (bent + steep * (1.0 - bent * bent))
            descriptor[rows, half * LANES : (half + 1) * LANES] = total / SLOTS
            descriptor[rows, ATOMS + half * LANES : ATOMS + (half + 1) * LANES] = tangent / SLOTS
            return carry

        lax.fori_loop(0, EMB // 16, embed, 0)

    first_copy.wait()
    inner = contract(descriptor[:], first_weight[:], (0, 0))
    first = jnp.tanh(inner[:ATOMS] + first_bias[:])
    forward[:ATOMS] = first
    forward[ATOMS:] = (1.0 - first * first) * inner[ATOMS:]
    upper, lower = halves(forward[:])
    features[: 2 * ATOMS] = upper
    features[2 * ATOMS :] = lower
    middle_copy.wait()
    outer = contract(forward[:], middle_weight[:], (1, 0))
    second = jnp.tanh(outer[:ATOMS] + middle_bias[:])
    bend = 1.0 - second * second
    second_dot = bend * outer[ATOMS:]
    own = lax.broadcasted_iota(jnp.int32, (4, ATOMS), 0) == species[:]
    readout = contract(own.astype(jnp.float32), energy_weight[:], (0, 0))
    slope = readout * bend
    slope_dot = -2.0 * readout * second * second_dot
    energy = readout * second
    force = -(readout * second_dot)
    sums = [jnp.zeros((1, HID), jnp.float32) for _ in range(OBS_DP)]
    for s in range(LOCAL_STRUCTS):
        rows = slice(s * STRUCT, (s + 1) * STRUCT)
        q = observed[s]
        is_energy = q == 0
        direct = halves(
            jnp.where(is_energy, slope[rows] * (weighting / STRUCT), slope_dot[rows] * -weighting)
        )
        through = halves(slope[rows] * -weighting)
        value = jnp.sum(
            jnp.where(is_energy, energy[rows] * (weighting / STRUCT), force[rows] * weighting),
            axis=0,
            keepdims=True,
        )
        for o in range(OBS_DP):
            columns = slice(o * HID, (o + 1) * HID)
            for kind, pair in enumerate((direct, through)):
                for part in range(2):
                    start = (1 - part) * 2 * ATOMS + kind * ATOMS + s * STRUCT
                    heads[start : start + STRUCT, columns] = jnp.where(
                        q == o, pair[part], jnp.bfloat16(0)
                    )
            sums[o] = sums[o] + jnp.where(q == o, value, 0.0)
    predicted[:] = jnp.zeros((8, LANES), jnp.float32)
    for o in range(OBS_DP):
        predicted[o : o + 1, :] = sums[o][:, :LANES] + sums[o][:, LANES:]
    jacobian[:] = lax.dot_general(
        features[:], heads[:], (((0,), (0,)), ((), ())), preferred_element_type=jnp.float32
    ) + lax.dot_general(
        features[: 2 * ATOMS],
        heads[2 * ATOMS :],
        (((0,), (0,)), ((), ())),
        preferred_element_type=jnp.float32,
    )
    for y in range(4):
        for z in range(4):
            pair = (z * 8 + y * 2) * 8
            ours = pl.multiple_of(pair + core * 8, 8)
            other = pl.multiple_of(pair + (1 - core) * 8, 8)
            mine[y, z] = jacobian[pl.ds(ours, 8), :]
            theirs[y, z] = jacobian[pl.ds(other, 8), :]
    line = middle_weight[pl.ds(block * 8 + group // 2, 1), :]
    kept[0:1] = jnp.where(group % 2 == 0, line[:, :LANES], line[:, LANES:])
    kept[1:2] = jnp.concatenate([targets[:], noise[:]], axis=1)
    kept[2:8] = jnp.zeros((6, LANES), jnp.float32)


def product_kernel(gathered, covariance, predicted, columns, sent):
    for i in range(8):
        for q in range(OBS_DP):
            columns[q * GROUPS : (q + 1) * GROUPS, i * HID : (i + 1) * HID] = gathered[
                :, i, q * HID : (q + 1) * HID
            ]
    product = contract(columns[:], covariance[0], (1, 1))
    for d in range(GROUPS):
        sent[d, :OBS] = product
        sent[d, OBS:] = predicted[:]


def gram_kernel(columns, products, sent):
    gram = jnp.zeros((OBS, OBS), jnp.float32)
    for d in range(GROUPS):
        gram = gram + contract(columns[:, d * ROWS : (d + 1) * ROWS], products[d, :OBS], (1, 1))
    half = OBS // 2
    values = jnp.sum(
        jnp.concatenate([products[:, OBS + q, :] for q in range(OBS_DP)], axis=0),
        axis=1,
        keepdims=True,
    )
    packed = jnp.concatenate(
        [
            gram[:half],
            gram[half:, half:],
            values[:half],
            values[half:],
            jnp.zeros((half, half - 2), jnp.float32),
        ],
        axis=1,
    )
    for k in range(8):
        sent[k] = packed


def summed_kernel(arrived, sent):
    total = arrived[0]
    for k in range(1, 8):
        total = total + arrived[k]
    for k in range(4):
        sent[k] = total


def update_kernel(
    place,
    arrived,
    products,
    covariance,
    kept,
    new_weights,
    new_covariance,
    wide,
    result,
    departures,
):
    group = place[2]
    half = OBS // 2
    packed = (arrived[0] + arrived[1]) + (arrived[2] + arrived[3])
    corner = packed[:, half:OBS]
    gram = jnp.concatenate(
        [
            packed[:, :OBS],
            jnp.concatenate([corner.T, packed[:, OBS : OBS + half]], axis=1),
        ],
        axis=0,
    )
    gram = 0.5 * (gram + gram.T)
    observed = jnp.concatenate([packed[:, 96:97], packed[:, 97:98]], axis=0)
    down = lax.broadcasted_iota(jnp.int32, (OBS, OBS), 0)
    across = lax.broadcasted_iota(jnp.int32, (OBS, OBS), 1)
    source = across == down % GROUPS * OBS_DP + down // GROUPS
    noise_here = jnp.sum(jnp.where(source, kept[1:2, OBS:], 0.0), axis=1, keepdims=True)
    target_here = jnp.sum(jnp.where(source, kept[1:2, :OBS], 0.0), axis=1, keepdims=True)
    identity = (down == across).astype(jnp.float32)
    gram = gram + jnp.where(down == across, noise_here, 0.0)
    work = jnp.concatenate([gram, identity], axis=1)
    strips = [work[8 * k : 8 * k + 8] for k in range(8)]
    sublane = lax.broadcasted_iota(jnp.int32, (8, LANES), 0)
    roots = []
    for k in range(8):
        active = range(k, 8)
        panel = [
            {r: jnp.broadcast_to(strips[r][:, 8 * k + j : 8 * k + j + 1], (8, LANES)) for r in active}
            for j in range(8)
        ]
        pivots = jnp.ones((8, LANES), jnp.float32)
        for j in range(8):
            pivot = jnp.broadcast_to(panel[j][k][j : j + 1], (8, LANES))
            pivots = jnp.where(sublane == j, pivot, pivots)
            inverse = 1.0 / pivot
            factor = {r: panel[j][r] * inverse for r in active}
            factor[k] = jnp.where(sublane > j, factor[k], 0.0)
            for n in range(j + 1, 8):
                head = jnp.broadcast_to(panel[n][k][j : j + 1], (8, LANES))
                for r in active:
                    panel[n][r] = panel[n][r] - factor[r] * head
            row = jnp.broadcast_to(strips[k][j : j + 1], (8, LANES))
            for r in active:
                strips[r] = strips[r] - factor[r] * row
        roots.append(strips[k] * lax.rsqrt(pivots))
    root = jnp.concatenate(roots, axis=0)[:, OBS:]
    for d in range(GROUPS):
        wide[:, d * ROWS : (d + 1) * ROWS] = products[d, :OBS]
    own = products[group, :OBS]
    gain = contract(root, contract(root, own, (1, 0)), (0, 0))
    new_weights[:] = kept[0:1] + jnp.sum(gain * (target_here - observed), axis=0, keepdims=True)
    turned = gain.T
    copies = []
    for c in range(4):
        columns = slice(c * ORDER // 4, (c + 1) * ORDER // 4)
        update = contract(turned, wide[:, columns], (1, 0))
        result[:, columns] = (covariance[0, :, columns] - update) / forgetting
        copy = pltpu.make_async_copy(
            result.at[:, columns], new_covariance.at[0, :, columns], departures.at[c]
        )
        copy.start()
        copies.append(copy)
    for copy in copies:
        copy.wait()


def exchanged(tiles, axes):
    return lax.all_to_all(tiles, axes, split_axis=0, concat_axis=0, tiled=True)


def local(
    positions,
    neighbours,
    atom_species,
    tagged_atom,
    observed_in,
    targets,
    noise_level,
    embed_scale,
    embed_shift,
    first_weight,
    first_bias,
    middle_weight,
    middle_bias,
    energy_weight,
    covariance,
    weighting,
):
    f32 = jnp.float32
    place = jnp.stack(
        [lax.axis_index("block_2"), lax.axis_index(BLOCK), lax.axis_index(DP)]
    ).astype(jnp.int32)
    mine, theirs, predicted, kept = pl.pallas_call(
        functools.partial(jacobian_kernel, weighting=weighting),
        out_shape=(
            jax.ShapeDtypeStruct((4, 4, 8, OBS_DP * HID), f32),
            jax.ShapeDtypeStruct((4, 4, 8, OBS_DP * HID), f32),
            jax.ShapeDtypeStruct((8, LANES), f32),
            jax.ShapeDtypeStruct((8, LANES), f32),
        ),
        in_specs=[SMEM] * 3 + [VMEM] * 5 + [HBM, VMEM, HBM] + [VMEM] * 4,
        out_specs=(VMEM, VMEM, VMEM, VMEM),
        scratch_shapes=[
            pltpu.VMEM((8, EMB, LANES), f32),
            pltpu.VMEM((EMB, 2 * ATOMS), f32),
            pltpu.VMEM((2 * ATOMS, HID), f32),
            pltpu.VMEM((4 * ATOMS, HID), jnp.bfloat16),
            pltpu.VMEM((4 * ATOMS, OBS_DP * HID), jnp.bfloat16),
            pltpu.VMEM((HID, OBS_DP * HID), f32),
            pltpu.VMEM((EMB, HID), f32),
            pltpu.VMEM((HID, HID), f32),
            pltpu.SemaphoreType.DMA((2,)),
        ],
        compiler_params=granted(12),
    )(
        place,
        tagged_atom,
        observed_in,
        positions,
        neighbours,
        atom_species[None],
        embed_scale,
        embed_shift,
        pltpu.with_memory_space_constraint(first_weight, pltpu.HBM),
        first_bias[None],
        pltpu.with_memory_space_constraint(middle_weight, pltpu.HBM),
        middle_bias[None],
        energy_weight,
        targets[None],
        noise_level[None],
    )
    partner = mine + lax.ppermute(theirs, "block_2", [(0, 1), (1, 0)])
    across_y = jnp.sum(exchanged(partner, "block_1"), axis=0)
    across_z = jnp.sum(exchanged(across_y, "block_0"), axis=0)
    gathered = exchanged(jnp.broadcast_to(across_z[None], (GROUPS, 8, OBS_DP * HID)), DP)
    columns, sent = pl.pallas_call(
        product_kernel,
        out_shape=(
            jax.ShapeDtypeStruct((OBS, ORDER), f32),
            jax.ShapeDtypeStruct((GROUPS, OBS + 8, ROWS), f32),
        ),
        in_specs=[VMEM] * 3,
        out_specs=(VMEM, VMEM),
        compiler_params=granted(8),
    )(gathered, covariance, predicted)
    products = exchanged(sent, DP)
    grams = pl.pallas_call(
        gram_kernel,
        out_shape=jax.ShapeDtypeStruct((8, OBS // 2, LANES), f32),
        in_specs=[VMEM] * 2,
        out_specs=VMEM,
        compiler_params=granted(8),
    )(columns, products)
    near = pl.pallas_call(
        summed_kernel,
        out_shape=jax.ShapeDtypeStruct((4, OBS // 2, LANES), f32),
        in_specs=[VMEM],
        out_specs=VMEM,
        compiler_params=granted(4),
    )(exchanged(grams, ("block_1", "block_2")))
    return pl.pallas_call(
        update_kernel,
        out_shape=(
            jax.ShapeDtypeStruct((1, ROWS), f32),
            jax.ShapeDtypeStruct((1, ROWS, ORDER), f32),
        ),
        in_specs=[SMEM] + [VMEM] * 4,
        out_specs=(VMEM, HBM),
        scratch_shapes=[
            pltpu.VMEM((OBS, ORDER), f32),
            pltpu.VMEM((ROWS, ORDER), f32),
            pltpu.SemaphoreType.DMA((4,)),
        ],
        compiler_params=granted(12),
    )(
        place,
        exchanged(near, "block_0"),
        products,
        covariance,
        kept,
    )


def solution(mesh):
    finer = Mesh(
        mesh.devices.reshape(4, 4, 4, 4, 2), ("dp_0", "dp_1", "block_0", "block_1", "block_2")
    )
    placed = (
        P(None, DP_BLOCK),
        P(None, DP_BLOCK),
        P(DP_BLOCK),
        P(DP_BLOCK),
        P(DP_BLOCK),
        P(),
        P(),
        P(),
        P(),
        P(),
        P(),
        P(),
        P(),
        P(),
        P(BLOCK, DP, None),
    )
    weighting = OBS / (LOCAL_STRUCTS * mesh.devices.size)
    return jax.shard_map(
        functools.partial(local, weighting=weighting),
        mesh=finer,
        in_specs=placed,
        out_specs=(P(BLOCK, DP), P(BLOCK, DP, None)),
        check_vma=False,
    )
```

```python
import functools

import jax
import jax.numpy as jnp
from jax import lax
from jax.experimental import pallas as pl
from jax.experimental.pallas import tpu as pltpu
from jax.sharding import Mesh
from jax.sharding import PartitionSpec as P

OBS = 64
GROUPS = 16
OBS_DP = 4
STRUCT = 32
LOCAL_STRUCTS = 8
ATOMS = 256
LANES = 128
HID = 256
EMB = 128
SLOTS = 16
ORDER = 2048
ROWS = 128
DP = ("dp_0", "dp_1")
BLOCK = ("block_0", "block_1", "block_2")
DP_BLOCK = ("dp_0", "dp_1", "block_0", "block_1", "block_2")

radial_width = 4.0
forgetting = 0.98
highest = lax.Precision.HIGHEST

VMEM = pl.BlockSpec(memory_space=pltpu.VMEM)
SMEM = pl.BlockSpec(memory_space=pltpu.SMEM)
HBM = pl.BlockSpec(memory_space=pltpu.HBM)


def granted(mib):
    return pltpu.CompilerParams(vmem_limit_bytes=mib * 1024 * 1024)


def contract(lhs, rhs, over):
    return lax.dot_general(
        lhs, rhs, ((over[:1], over[1:]), ((), ())), precision=highest, preferred_element_type=jnp.float32
    )


def halves(values):
    upper = values.astype(jnp.bfloat16)
    return upper, (values - upper.astype(jnp.float32)).astype(jnp.bfloat16)


def stacked(values, order):
    pair = halves(values)
    return jnp.concatenate([pair[n] for n in order], axis=0)


def plain(lhs, rhs, over):
    return lax.dot_general(
        lhs, rhs, ((over[:1], over[1:]), ((), ())), preferred_element_type=jnp.float32
    )


def along_lanes(row, at):
    return jnp.take_along_axis(
        jnp.broadcast_to(row, at.shape), at, axis=1, mode="promise_in_bounds"
    )


def jacobian_kernel(
    place,
    tagged,
    observed,
    positions,
    neighbours,
    species,
    scale,
    shift,
    first_source,
    first_bias,
    middle_source,
    middle_bias,
    energy_weight,
    targets,
    noise,
    mine,
    theirs,
    predicted,
    kept,
    tables,
    descriptor,
    features,
    jacobian,
    first_weight,
    middle_weight,
    arrivals,
    weighting,
):
    core, block, group = place[0], place[1], place[2]
    first_copy = pltpu.make_async_copy(first_source, first_weight, arrivals.at[0])
    middle_copy = pltpu.make_async_copy(middle_source, middle_weight, arrivals.at[1])
    first_copy.start()
    middle_copy.start()
    for kind, table in enumerate((scale, shift)):
        columns = table[:].T
        for s in range(4):
            tables[kind * 4 + s] = jnp.broadcast_to(columns[:, s : s + 1], (EMB, LANES))
    lane = lax.broadcasted_iota(jnp.int32, (SLOTS, LANES), 1)
    for half in range(2):
        lanes = slice(half * LANES, (half + 1) * LANES)
        tag = jnp.zeros((SLOTS, LANES), jnp.int32)
        part = jnp.zeros((SLOTS, LANES), jnp.int32)
        for s in range(4):
            here = lane // STRUCT == s
            tag = jnp.where(here, tagged[half * 4 + s], tag)
            part = jnp.where(here, observed[half * 4 + s], part)
        listed = neighbours[:, lanes]
        within = jnp.minimum(listed, STRUCT - 1)
        at = lane // STRUCT * STRUCT + within
        distance_sq = jnp.zeros((SLOTS, LANES), jnp.float32)
        chosen = jnp.zeros((SLOTS, LANES), jnp.float32)
        for c in range(3):
            row = positions[c : c + 1, lanes]
            displace = along_lanes(row, at) - row
            distance_sq = distance_sq + displace * displace
            chosen = jnp.where(part == c + 1, displace, chosen)
        radial = jnp.exp(-distance_sq / radial_width) * (listed < STRUCT).astype(jnp.float32)
        moved = (within == tag).astype(jnp.float32) - (lane % STRUCT == tag).astype(jnp.float32)
        radial_dot = radial * (-2.0 / radial_width) * chosen * moved
        near = along_lanes(species[:, lanes], at)
        odd = (near & 1) == 1
        upper = near >= 2

        def embed(step, carry, half=half, radial=radial, radial_dot=radial_dot, odd=odd, upper=upper):
            start = pl.multiple_of(step * 16, 16)
            rows = pl.ds(start, 16)
            held = [tables[n, rows, :] for n in range(8)]
            total = jnp.zeros((16, LANES), jnp.float32)
            tangent = jnp.zeros((16, LANES), jnp.float32)
            for k in range(SLOTS):
                r = jnp.broadcast_to(radial[k : k + 1], (16, LANES))
                r_dot = jnp.broadcast_to(radial_dot[k : k + 1], (16, LANES))
                is_odd = jnp.broadcast_to(odd[k : k + 1], (16, LANES))
                is_upper = jnp.broadcast_to(upper[k : k + 1], (16, LANES))
                slope = jnp.where(
                    is_upper,
                    jnp.where(is_odd, held[3], held[2]),
                    jnp.where(is_odd, held[1], held[0]),
                )
                offset = jnp.where(
                    is_upper,
                    jnp.where(is_odd, held[7], held[6]),
                    jnp.where(is_odd, held[5], held[4]),
                )
                steep = r * slope
                bent = jnp.tanh(steep + offset)
                total = total + r * bent
                tangent = tangent + r_dot * (bent + steep * (1.0 - bent * bent))
            descriptor[rows, half * LANES : (half + 1) * LANES] = total / SLOTS
            descriptor[rows, ATOMS + half * LANES : ATOMS + (half + 1) * LANES] = tangent / SLOTS
            return carry

        lax.fori_loop(0, EMB // 16, embed, 0)

    first_copy.wait()
    inner = plain(
        stacked(descriptor[:], (0, 1, 0)), stacked(first_weight[:], (0, 0, 1)), (0, 0)
    )
    first = jnp.tanh(inner[:ATOMS] + first_bias[:])
    upper, lower = halves(
        jnp.concatenate([first, (1.0 - first * first) * inner[ATOMS:]], axis=0)
    )
    for s in range(LOCAL_STRUCTS):
        for n, piece in enumerate((upper, upper, lower, lower)):
            source = n % 2 * ATOMS + s * STRUCT
            start = (s * 4 + n) * STRUCT
            features[start : start + STRUCT] = piece[source : source + STRUCT]
    middle_copy.wait()
    wide, narrow = halves(middle_weight[:])
    outer = (plain(upper, narrow, (1, 0)) + plain(lower, wide, (1, 0))) + plain(
        upper, wide, (1, 0)
    )
    second = jnp.tanh(outer[:ATOMS] + middle_bias[:])
    bend = 1.0 - second * second
    second_dot = bend * outer[ATOMS:]
    own = lax.broadcasted_iota(jnp.int32, (4, ATOMS), 0) == species[:]
    readout = contract(own.astype(jnp.float32), energy_weight[:], (0, 0))
    slope = readout * bend
    slope_dot = -2.0 * readout * second * second_dot
    energy = readout * second
    force = -(readout * second_dot)
    turned = features[:].T
    jacobian[:] = jnp.zeros((OBS_DP, HID, HID), jnp.float32)
    sums = [jnp.zeros((1, HID), jnp.float32) for _ in range(OBS_DP)]
    for s in range(LOCAL_STRUCTS):
        rows = slice(s * STRUCT, (s + 1) * STRUCT)
        q = observed[s]
        is_energy = q == 0
        head, tail = halves(
            jnp.concatenate(
                [
                    jnp.where(
                        is_energy, slope[rows] * (weighting / STRUCT), slope_dot[rows] * -weighting
                    ),
                    slope[rows] * -weighting,
                ],
                axis=0,
            )
        )
        value = jnp.sum(
            jnp.where(is_energy, energy[rows] * (weighting / STRUCT), force[rows] * weighting),
            axis=0,
            keepdims=True,
        )
        for o in range(OBS_DP):
            sums[o] = sums[o] + jnp.where(q == o, value, 0.0)
        lanes = turned[:, s * 4 * STRUCT : (s + 1) * 4 * STRUCT]
        jacobian[q] += plain(
            jnp.concatenate([lanes, lanes], axis=1),
            jnp.concatenate([head, head, tail, jnp.zeros_like(tail)], axis=0),
            (1, 0),
        )
    predicted[:] = jnp.zeros((8, LANES), jnp.float32)
    for o in range(OBS_DP):
        predicted[o : o + 1, :] = sums[o][:, :LANES] + sums[o][:, LANES:]
    for y in range(4):
        for z in range(4):
            pair = (z * 8 + y * 2) * 8
            ours = pl.multiple_of(pair + core * 8, 8)
            other = pl.multiple_of(pair + (1 - core) * 8, 8)
            for q in range(OBS_DP):
                columns = slice(q * HID, (q + 1) * HID)
                mine[y, z, :, columns] = jacobian[q, pl.ds(ours, 8), :]
                theirs[y, z, :, columns] = jacobian[q, pl.ds(other, 8), :]
    line = middle_weight[pl.ds(block * 8 + group // 2, 1), :]
    kept[0:1] = jnp.where(group % 2 == 0, line[:, :LANES], line[:, LANES:])
    kept[1:2] = jnp.concatenate([targets[:], noise[:]], axis=1)
    kept[2:8] = jnp.zeros((6, LANES), jnp.float32)


def product_kernel(gathered, covariance, predicted, columns, sent):
    for i in range(8):
        for q in range(OBS_DP):
            columns[q * GROUPS : (q + 1) * GROUPS, i * HID : (i + 1) * HID] = gathered[
                :, i, q * HID : (q + 1) * HID
            ]
    product = contract(columns[:], covariance[0], (1, 1))
    for d in range(GROUPS):
        sent[d, :OBS] = product
        sent[d, OBS:] = predicted[:]


def gram_kernel(columns, products, sent):
    gram = jnp.zeros((OBS, OBS), jnp.float32)
    for d in range(GROUPS):
        gram = gram + contract(columns[:, d * ROWS : (d + 1) * ROWS], products[d, :OBS], (1, 1))
    half = OBS // 2
    values = jnp.sum(
        jnp.concatenate([products[:, OBS + q, :] for q in range(OBS_DP)], axis=0),
        axis=1,
        keepdims=True,
    )
    packed = jnp.concatenate(
        [
            gram[:half],
            gram[half:, half:],
            values[:half],
            values[half:],
            jnp.zeros((half, half - 2), jnp.float32),
        ],
        axis=1,
    )
    for k in range(8):
        sent[k] = packed


def summed_kernel(arrived, sent):
    total = arrived[0]
    for k in range(1, 8):
        total = total + arrived[k]
    for k in range(4):
        sent[k] = total


def update_kernel(
    place,
    arrived,
    products,
    covariance,
    kept,
    new_weights,
    new_covariance,
    wide,
    result,
    departures,
):
    group = place[2]
    half = OBS // 2
    packed = (arrived[0] + arrived[1]) + (arrived[2] + arrived[3])
    corner = packed[:, half:OBS]
    gram = jnp.concatenate(
        [
            packed[:, :OBS],
            jnp.concatenate([corner.T, packed[:, OBS : OBS + half]], axis=1),
        ],
        axis=0,
    )
    gram = 0.5 * (gram + gram.T)
    observed = jnp.concatenate([packed[:, 96:97], packed[:, 97:98]], axis=0)
    down = lax.broadcasted_iota(jnp.int32, (OBS, OBS), 0)
    across = lax.broadcasted_iota(jnp.int32, (OBS, OBS), 1)
    source = across == down % GROUPS * OBS_DP + down // GROUPS
    noise_here = jnp.sum(jnp.where(source, kept[1:2, OBS:], 0.0), axis=1, keepdims=True)
    target_here = jnp.sum(jnp.where(source, kept[1:2, :OBS], 0.0), axis=1, keepdims=True)
    identity = (down == across).astype(jnp.float32)
    gram = gram + jnp.where(down == across, noise_here, 0.0)
    work = jnp.concatenate([gram, identity], axis=1)
    strips = [work[8 * k : 8 * k + 8] for k in range(8)]
    sublane = lax.broadcasted_iota(jnp.int32, (8, LANES), 0)
    roots = []
    for k in range(8):
        active = range(k, 8)
        panel = [
            {r: jnp.broadcast_to(strips[r][:, 8 * k + j : 8 * k + j + 1], (8, LANES)) for r in active}
            for j in range(8)
        ]
        pivots = jnp.ones((8, LANES), jnp.float32)
        for j in range(0, 8, 2):
            left, right = panel[j], panel[j + 1]
            top = jnp.broadcast_to(left[k][j : j + 1], (8, LANES))
            side = jnp.broadcast_to(right[k][j : j + 1], (8, LANES))
            corner = jnp.broadcast_to(right[k][j + 1 : j + 2], (8, LANES))
            area = top * corner - side * side
            inverse = 1.0 / area
            one = {r: (left[r] * corner - right[r] * side) * inverse for r in active}
            two = {r: (right[r] * top - left[r] * side) * inverse for r in active}
            one[k] = jnp.where(sublane > j + 1, one[k], 0.0)
            two[k] = jnp.where(sublane > j + 1, two[k], 0.0)
            for n in range(j + 2, 8):
                head = jnp.broadcast_to(panel[n][k][j : j + 1], (8, LANES))
                tail = jnp.broadcast_to(panel[n][k][j + 1 : j + 2], (8, LANES))
                for r in active:
                    panel[n][r] = panel[n][r] - (one[r] * head + two[r] * tail)
            head = jnp.broadcast_to(strips[k][j : j + 1], (8, LANES))
            tail = jnp.broadcast_to(strips[k][j + 1 : j + 2], (8, LANES))
            for r in active:
                strips[r] = strips[r] - (one[r] * head + two[r] * tail)
            ratio = 1.0 / top
            strips[k] = jnp.where(sublane == j + 1, strips[k] - side * ratio * head, strips[k])
            pivots = jnp.where(sublane == j, top, pivots)
            pivots = jnp.where(sublane == j + 1, area * ratio, pivots)
        roots.append(strips[k] * lax.rsqrt(pivots))
    root = jnp.concatenate(roots, axis=0)[:, OBS:]
    for d in range(GROUPS):
        wide[:, d * ROWS : (d + 1) * ROWS] = stacked(products[d, :OBS], (0, 0, 1))
    own = products[group, :OBS]
    gain = contract(root, contract(root, own, (1, 0)), (0, 0))
    new_weights[:] = kept[0:1] + jnp.sum(gain * (target_here - observed), axis=0, keepdims=True)
    turned = stacked(gain, (0, 1, 0))
    copies = []
    for c in range(4):
        columns = slice(c * ORDER // 4, (c + 1) * ORDER // 4)
        update = plain(turned, wide[:, columns], (0, 0))
        result[:, columns] = (covariance[0, :, columns] - update) / forgetting
        copy = pltpu.make_async_copy(
            result.at[:, columns], new_covariance.at[0, :, columns], departures.at[c]
        )
        copy.start()
        copies.append(copy)
    for copy in copies:
        copy.wait()


def exchanged(tiles, axes):
    return lax.all_to_all(tiles, axes, split_axis=0, concat_axis=0, tiled=True)


def local(
    positions,
    neighbours,
    atom_species,
    tagged_atom,
    observed_in,
    targets,
    noise_level,
    embed_scale,
    embed_shift,
    first_weight,
    first_bias,
    middle_weight,
    middle_bias,
    energy_weight,
    covariance,
    weighting,
):
    f32 = jnp.float32
    place = jnp.stack(
        [lax.axis_index("block_2"), lax.axis_index(BLOCK), lax.axis_index(DP)]
    ).astype(jnp.int32)
    mine, theirs, predicted, kept = pl.pallas_call(
        functools.partial(jacobian_kernel, weighting=weighting),
        out_shape=(
            jax.ShapeDtypeStruct((4, 4, 8, OBS_DP * HID), f32),
            jax.ShapeDtypeStruct((4, 4, 8, OBS_DP * HID), f32),
            jax.ShapeDtypeStruct((8, LANES), f32),
            jax.ShapeDtypeStruct((8, LANES), f32),
        ),
        in_specs=[SMEM] * 3 + [VMEM] * 5 + [HBM, VMEM, HBM] + [VMEM] * 4,
        out_specs=(VMEM, VMEM, VMEM, VMEM),
        scratch_shapes=[
            pltpu.VMEM((8, EMB, LANES), f32),
            pltpu.VMEM((EMB, 2 * ATOMS), f32),
            pltpu.VMEM((4 * ATOMS, HID), jnp.bfloat16),
            pltpu.VMEM((OBS_DP, HID, HID), f32),
            pltpu.VMEM((EMB, HID), f32),
            pltpu.VMEM((HID, HID), f32),
            pltpu.SemaphoreType.DMA((2,)),
        ],
        compiler_params=granted(12),
    )(
        place,
        tagged_atom,
        observed_in,
        positions,
        neighbours,
        atom_species[None],
        embed_scale,
        embed_shift,
        pltpu.with_memory_space_constraint(first_weight, pltpu.HBM),
        first_bias[None],
        pltpu.with_memory_space_constraint(middle_weight, pltpu.HBM),
        middle_bias[None],
        energy_weight,
        targets[None],
        noise_level[None],
    )
    partner = mine + lax.ppermute(theirs, "block_2", [(0, 1), (1, 0)])
    across_y = jnp.sum(exchanged(partner, "block_1"), axis=0)
    across_z = jnp.sum(exchanged(across_y, "block_0"), axis=0)
    gathered = exchanged(jnp.broadcast_to(across_z[None], (GROUPS, 8, OBS_DP * HID)), DP)
    columns, sent = pl.pallas_call(
        product_kernel,
        out_shape=(
            jax.ShapeDtypeStruct((OBS, ORDER), f32),
            jax.ShapeDtypeStruct((GROUPS, OBS + 8, ROWS), f32),
        ),
        in_specs=[VMEM] * 3,
        out_specs=(VMEM, VMEM),
        compiler_params=granted(8),
    )(gathered, covariance, predicted)
    products = exchanged(sent, DP)
    grams = pl.pallas_call(
        gram_kernel,
        out_shape=jax.ShapeDtypeStruct((8, OBS // 2, LANES), f32),
        in_specs=[VMEM] * 2,
        out_specs=VMEM,
        compiler_params=granted(8),
    )(columns, products)
    near = pl.pallas_call(
        summed_kernel,
        out_shape=jax.ShapeDtypeStruct((4, OBS // 2, LANES), f32),
        in_specs=[VMEM],
        out_specs=VMEM,
        compiler_params=granted(4),
    )(exchanged(grams, ("block_1", "block_2")))
    return pl.pallas_call(
        update_kernel,
        out_shape=(
            jax.ShapeDtypeStruct((1, ROWS), f32),
            jax.ShapeDtypeStruct((1, ROWS, ORDER), f32),
        ),
        in_specs=[SMEM] + [VMEM] * 4,
        out_specs=(VMEM, HBM),
        scratch_shapes=[
            pltpu.VMEM((3 * OBS, ORDER), jnp.bfloat16),
            pltpu.VMEM((ROWS, ORDER), f32),
            pltpu.SemaphoreType.DMA((4,)),
        ],
        compiler_params=granted(12),
    )(
        place,
        exchanged(near, "block_0"),
        products,
        covariance,
        kept,
    )


def solution(mesh):
    finer = Mesh(
        mesh.devices.reshape(4, 4, 4, 4, 2), ("dp_0", "dp_1", "block_0", "block_1", "block_2")
    )
    placed = (
        P(None, DP_BLOCK),
        P(None, DP_BLOCK),
        P(DP_BLOCK),
        P(DP_BLOCK),
        P(DP_BLOCK),
        P(),
        P(),
        P(),
        P(),
        P(),
        P(),
        P(),
        P(),
        P(),
        P(BLOCK, DP, None),
    )
    weighting = OBS / (LOCAL_STRUCTS * mesh.devices.size)
    return jax.shard_map(
        functools.partial(local, weighting=weighting),
        mesh=finer,
        in_specs=placed,
        out_specs=(P(BLOCK, DP), P(BLOCK, DP, None)),
        check_vma=False,
    )
```

```python
import functools

import jax
import jax.numpy as jnp
from jax import lax
from jax.experimental import pallas as pl
from jax.experimental.pallas import tpu as pltpu
from jax.sharding import Mesh
from jax.sharding import PartitionSpec as P

OBS = 64
GROUPS = 16
OBS_DP = 4
STRUCT = 32
LOCAL_STRUCTS = 8
ATOMS = 256
LANES = 128
HID = 256
EMB = 128
SLOTS = 16
ORDER = 2048
ROWS = 128
DP = ("dp_0", "dp_1")
BLOCK = ("block_0", "block_1", "block_2")
DP_BLOCK = ("dp_0", "dp_1", "block_0", "block_1", "block_2")

radial_width = 4.0
forgetting = 0.98
highest = lax.Precision.HIGHEST

VMEM = pl.BlockSpec(memory_space=pltpu.VMEM)
SMEM = pl.BlockSpec(memory_space=pltpu.SMEM)
HBM = pl.BlockSpec(memory_space=pltpu.HBM)


def granted(mib):
    return pltpu.CompilerParams(vmem_limit_bytes=mib * 1024 * 1024)


def contract(lhs, rhs, over):
    return lax.dot_general(
        lhs, rhs, ((over[:1], over[1:]), ((), ())), precision=highest, preferred_element_type=jnp.float32
    )


def halves(values):
    upper = values.astype(jnp.bfloat16)
    return upper, (values - upper.astype(jnp.float32)).astype(jnp.bfloat16)


def stacked(values, order):
    pair = halves(values)
    return jnp.concatenate([pair[n] for n in order], axis=0)


def plain(lhs, rhs, over):
    return lax.dot_general(
        lhs, rhs, ((over[:1], over[1:]), ((), ())), preferred_element_type=jnp.float32
    )


def along_lanes(row, at):
    return jnp.take_along_axis(
        jnp.broadcast_to(row, at.shape), at, axis=1, mode="promise_in_bounds"
    )


def jacobian_kernel(
    tags,
    parts,
    observed_source,
    positions,
    neighbours,
    species,
    scale,
    shift,
    first_source,
    first_bias,
    middle_source,
    middle_bias,
    energy_weight,
    targets,
    noise,
    mine,
    theirs,
    predicted,
    kept,
    tables,
    descriptor,
    features,
    jacobian,
    first_weight,
    middle_weight,
    observed,
    arrivals,
    weighting,
):
    core = lax.axis_index("block_2")
    block, group = lax.axis_index(BLOCK), lax.axis_index(DP)
    observed_copy = pltpu.make_async_copy(observed_source, observed, arrivals.at[2])
    observed_copy.start()
    first_copy = pltpu.make_async_copy(first_source, first_weight, arrivals.at[0])
    middle_copy = pltpu.make_async_copy(middle_source, middle_weight, arrivals.at[1])
    first_copy.start()
    middle_copy.start()
    for kind, table in enumerate((scale, shift)):
        columns = table[:].T
        for s in range(4):
            tables[kind * 4 + s] = jnp.broadcast_to(columns[:, s : s + 1], (EMB, LANES))
    lane = lax.broadcasted_iota(jnp.int32, (SLOTS, LANES), 1)
    for half in range(2):
        lanes = slice(half * LANES, (half + 1) * LANES)
        tag = jnp.zeros((SLOTS, LANES), jnp.int32)
        part = jnp.zeros((SLOTS, LANES), jnp.int32)
        for s in range(4):
            here = lane // STRUCT == s
            own = slice(half * 4 + s, half * 4 + s + 1)
            tag = jnp.where(here, tags[:, own], tag)
            part = jnp.where(here, parts[:, own], part)
        listed = neighbours[:, lanes]
        within = jnp.minimum(listed, STRUCT - 1)
        at = lane // STRUCT * STRUCT + within
        distance_sq = jnp.zeros((SLOTS, LANES), jnp.float32)
        chosen = jnp.zeros((SLOTS, LANES), jnp.float32)
        for c in range(3):
            row = positions[c : c + 1, lanes]
            displace = along_lanes(row, at) - row
            distance_sq = distance_sq + displace * displace
            chosen = jnp.where(part == c + 1, displace, chosen)
        radial = jnp.exp(-distance_sq / radial_width) * (listed < STRUCT).astype(jnp.float32)
        moved = (within == tag).astype(jnp.float32) - (lane % STRUCT == tag).astype(jnp.float32)
        radial_dot = radial * (-2.0 / radial_width) * chosen * moved
        near = along_lanes(species[:, lanes], at)
        odd = (near & 1) == 1
        upper = near >= 2

        def embed(step, carry, half=half, radial=radial, radial_dot=radial_dot, odd=odd, upper=upper):
            start = pl.multiple_of(step * 16, 16)
            rows = pl.ds(start, 16)
            held = [tables[n, rows, :] for n in range(8)]
            total = jnp.zeros((16, LANES), jnp.float32)
            tangent = jnp.zeros((16, LANES), jnp.float32)
            for k in range(SLOTS):
                r = jnp.broadcast_to(radial[k : k + 1], (16, LANES))
                r_dot = jnp.broadcast_to(radial_dot[k : k + 1], (16, LANES))
                is_odd = jnp.broadcast_to(odd[k : k + 1], (16, LANES))
                is_upper = jnp.broadcast_to(upper[k : k + 1], (16, LANES))
                slope = jnp.where(
                    is_upper,
                    jnp.where(is_odd, held[3], held[2]),
                    jnp.where(is_odd, held[1], held[0]),
                )
                offset = jnp.where(
                    is_upper,
                    jnp.where(is_odd, held[7], held[6]),
                    jnp.where(is_odd, held[5], held[4]),
                )
                steep = r * slope
                bent = jnp.tanh(steep + offset)
                total = total + r * bent
                tangent = tangent + r_dot * (bent + steep * (1.0 - bent * bent))
            descriptor[rows, half * LANES : (half + 1) * LANES] = total / SLOTS
            descriptor[rows, ATOMS + half * LANES : ATOMS + (half + 1) * LANES] = tangent / SLOTS
            return carry

        lax.fori_loop(0, EMB // 16, embed, 0)

    first_copy.wait()
    inner = plain(
        stacked(descriptor[:], (0, 1, 0)), stacked(first_weight[:], (0, 0, 1)), (0, 0)
    )
    first = jnp.tanh(inner[:ATOMS] + first_bias[:])
    upper, lower = halves(
        jnp.concatenate([first, (1.0 - first * first) * inner[ATOMS:]], axis=0)
    )
    for s in range(LOCAL_STRUCTS):
        for n, piece in enumerate((upper, upper, lower, lower)):
            source = n % 2 * ATOMS + s * STRUCT
            start = (s * 4 + n) * STRUCT
            features[start : start + STRUCT] = piece[source : source + STRUCT]
    middle_copy.wait()
    wide, narrow = halves(middle_weight[:])
    outer = (plain(upper, narrow, (1, 0)) + plain(lower, wide, (1, 0))) + plain(
        upper, wide, (1, 0)
    )
    second = jnp.tanh(outer[:ATOMS] + middle_bias[:])
    bend = 1.0 - second * second
    second_dot = bend * outer[ATOMS:]
    own = lax.broadcasted_iota(jnp.int32, (4, ATOMS), 0) == species[:]
    readout = contract(own.astype(jnp.float32), energy_weight[:], (0, 0))
    slope = readout * bend
    slope_dot = -2.0 * readout * second * second_dot
    energy = readout * second
    force = -(readout * second_dot)
    turned = features[:].T
    observed_copy.wait()
    jacobian[:] = jnp.zeros((OBS_DP, HID, HID), jnp.float32)
    sums = [jnp.zeros((1, HID), jnp.float32) for _ in range(OBS_DP)]
    for s in range(LOCAL_STRUCTS):
        rows = slice(s * STRUCT, (s + 1) * STRUCT)
        q = observed[s]
        is_energy = q == 0
        head, tail = halves(
            jnp.concatenate(
                [
                    jnp.where(
                        is_energy, slope[rows] * (weighting / STRUCT), slope_dot[rows] * -weighting
                    ),
                    slope[rows] * -weighting,
                ],
                axis=0,
            )
        )
        value = jnp.sum(
            jnp.where(is_energy, energy[rows] * (weighting / STRUCT), force[rows] * weighting),
            axis=0,
            keepdims=True,
        )
        for o in range(OBS_DP):
            sums[o] = sums[o] + jnp.where(q == o, value, 0.0)
        lanes = turned[:, s * 4 * STRUCT : (s + 1) * 4 * STRUCT]
        jacobian[q] += plain(
            jnp.concatenate([lanes, lanes], axis=1),
            jnp.concatenate([head, head, tail, jnp.zeros_like(tail)], axis=0),
            (1, 0),
        )
    predicted[:] = jnp.zeros((8, LANES), jnp.float32)
    for o in range(OBS_DP):
        predicted[o : o + 1, :] = sums[o][:, :LANES] + sums[o][:, LANES:]
    for y in range(4):
        for z in range(4):
            pair = (z * 8 + y * 2) * 8
            ours = pl.multiple_of(pair + core * 8, 8)
            other = pl.multiple_of(pair + (1 - core) * 8, 8)
            for q in range(OBS_DP):
                columns = slice(q * HID, (q + 1) * HID)
                mine[y, z, :, columns] = jacobian[q, pl.ds(ours, 8), :]
                theirs[y, z, :, columns] = jacobian[q, pl.ds(other, 8), :]
    line = middle_weight[pl.ds(block * 8 + group // 2, 1), :]
    kept[0:1] = jnp.where(group % 2 == 0, line[:, :LANES], line[:, LANES:])
    kept[1:2] = jnp.concatenate([targets[:], noise[:]], axis=1)
    kept[2:8] = jnp.zeros((6, LANES), jnp.float32)


def product_kernel(gathered, covariance, predicted, columns, sent):
    for i in range(8):
        for q in range(OBS_DP):
            columns[q * GROUPS : (q + 1) * GROUPS, i * HID : (i + 1) * HID] = gathered[
                :, i, q * HID : (q + 1) * HID
            ]
    product = contract(columns[:], covariance[0], (1, 1))
    for d in range(GROUPS):
        sent[d, :OBS] = product
        sent[d, OBS:] = predicted[:]


def gram_kernel(columns, products, sent, wide):
    for d in range(GROUPS):
        wide[:, d * ROWS : (d + 1) * ROWS] = products[d, :OBS]
    gram = contract(columns[:], wide[:], (1, 1))
    half = OBS // 2
    values = jnp.sum(
        jnp.concatenate([products[:, OBS + q, :] for q in range(OBS_DP)], axis=0),
        axis=1,
        keepdims=True,
    )
    packed = jnp.concatenate(
        [
            gram[:half],
            gram[half:, half:],
            values[:half],
            values[half:],
            jnp.zeros((half, half - 2), jnp.float32),
        ],
        axis=1,
    )
    for k in range(8):
        sent[k] = packed


def summed_kernel(arrived, sent):
    total = arrived[0]
    for k in range(1, 8):
        total = total + arrived[k]
    for k in range(4):
        sent[k] = total


def update_kernel(
    arrived,
    products,
    sent,
    covariance,
    kept,
    new_weights,
    new_covariance,
    wide,
    result,
    departures,
):
    half = OBS // 2
    packed = (arrived[0] + arrived[1]) + (arrived[2] + arrived[3])
    gram = jnp.concatenate(
        [
            jnp.concatenate([packed[:, :half], 2.0 * packed[:, half:OBS]], axis=1),
            jnp.concatenate(
                [jnp.zeros((half, half), jnp.float32), packed[:, OBS : OBS + half]], axis=1
            ),
        ],
        axis=0,
    )
    gram = 0.5 * (gram + gram.T)
    observed = jnp.concatenate([packed[:, 96:97], packed[:, 97:98]], axis=0)
    down = lax.broadcasted_iota(jnp.int32, (OBS, OBS), 0)
    across = lax.broadcasted_iota(jnp.int32, (OBS, OBS), 1)
    source = across == down % GROUPS * OBS_DP + down // GROUPS
    noise_here = jnp.sum(jnp.where(source, kept[1:2, OBS:], 0.0), axis=1, keepdims=True)
    target_here = jnp.sum(jnp.where(source, kept[1:2, :OBS], 0.0), axis=1, keepdims=True)
    identity = (down == across).astype(jnp.float32)
    gram = gram + jnp.where(down == across, noise_here, 0.0)
    work = jnp.concatenate([gram, identity], axis=1)
    strips = [work[8 * k : 8 * k + 8] for k in range(8)]
    sublane = lax.broadcasted_iota(jnp.int32, (8, LANES), 0)
    roots = []
    for k in range(0, 8, 2):
        active = range(k, 8)
        panel = [
            {r: jnp.broadcast_to(strips[r][:, 8 * k + j : 8 * k + j + 1], (8, LANES)) for r in active}
            for j in range(16)
        ]
        pivots = {k: jnp.ones((8, LANES), jnp.float32), k + 1: jnp.ones((8, LANES), jnp.float32)}
        for j in range(0, 16, 2):
            c, i = k + j // 8, j % 8
            left, right = panel[j], panel[j + 1]
            live = range(c, 8)
            top = jnp.broadcast_to(left[c][i : i + 1], (8, LANES))
            side = jnp.broadcast_to(right[c][i : i + 1], (8, LANES))
            corner = jnp.broadcast_to(right[c][i + 1 : i + 2], (8, LANES))
            area = top * corner - side * side
            inverse = 1.0 / area
            one = {r: (left[r] * corner - right[r] * side) * inverse for r in live}
            two = {r: (right[r] * top - left[r] * side) * inverse for r in live}
            one[c] = jnp.where(sublane > i + 1, one[c], 0.0)
            two[c] = jnp.where(sublane > i + 1, two[c], 0.0)
            for n in range(j + 2, 16):
                head = jnp.broadcast_to(panel[n][c][i : i + 1], (8, LANES))
                tail = jnp.broadcast_to(panel[n][c][i + 1 : i + 2], (8, LANES))
                for r in live:
                    panel[n][r] = panel[n][r] - (one[r] * head + two[r] * tail)
            head = jnp.broadcast_to(strips[c][i : i + 1], (8, LANES))
            tail = jnp.broadcast_to(strips[c][i + 1 : i + 2], (8, LANES))
            for r in live:
                strips[r] = strips[r] - (one[r] * head + two[r] * tail)
            ratio = 1.0 / top
            strips[c] = jnp.where(sublane == i + 1, strips[c] - side * ratio * head, strips[c])
            pivots[c] = jnp.where(sublane == i, top, pivots[c])
            pivots[c] = jnp.where(sublane == i + 1, area * ratio, pivots[c])
        for c in (k, k + 1):
            roots.append(strips[c] * lax.rsqrt(pivots[c]))
    root = jnp.concatenate(roots, axis=0)[:, OBS:]
    for d in range(GROUPS):
        wide[:, d * ROWS : (d + 1) * ROWS] = stacked(products[d, :OBS], (0, 0, 1))
    own = sent[0, :OBS]
    gain = contract(root, contract(root, own, (1, 0)), (0, 0))
    new_weights[:] = kept[0:1] + jnp.sum(gain * (target_here - observed), axis=0, keepdims=True)
    turned = stacked(gain, (0, 1, 0))
    copies = []
    for c in range(4):
        columns = slice(c * ORDER // 4, (c + 1) * ORDER // 4)
        update = plain(turned, wide[:, columns], (0, 0))
        result[:, columns] = (covariance[0, :, columns] - update) / forgetting
        copy = pltpu.make_async_copy(
            result.at[:, columns], new_covariance.at[0, :, columns], departures.at[c]
        )
        copy.start()
        copies.append(copy)
    for copy in copies:
        copy.wait()


def exchanged(tiles, axes):
    return lax.all_to_all(tiles, axes, split_axis=0, concat_axis=0, tiled=True)


def local(
    positions,
    neighbours,
    atom_species,
    tagged_atom,
    observed_in,
    targets,
    noise_level,
    embed_scale,
    embed_shift,
    first_weight,
    first_bias,
    middle_weight,
    middle_bias,
    energy_weight,
    covariance,
    weighting,
):
    f32 = jnp.float32
    mine, theirs, predicted, kept = pl.pallas_call(
        functools.partial(jacobian_kernel, weighting=weighting),
        out_shape=(
            jax.ShapeDtypeStruct((4, 4, 8, OBS_DP * HID), f32),
            jax.ShapeDtypeStruct((4, 4, 8, OBS_DP * HID), f32),
            jax.ShapeDtypeStruct((8, LANES), f32),
            jax.ShapeDtypeStruct((8, LANES), f32),
        ),
        in_specs=[VMEM, VMEM, HBM] + [VMEM] * 5 + [HBM, VMEM, HBM] + [VMEM] * 4,
        out_specs=(VMEM, VMEM, VMEM, VMEM),
        scratch_shapes=[
            pltpu.VMEM((8, EMB, LANES), f32),
            pltpu.VMEM((EMB, 2 * ATOMS), f32),
            pltpu.VMEM((4 * ATOMS, HID), jnp.bfloat16),
            pltpu.VMEM((OBS_DP, HID, HID), f32),
            pltpu.VMEM((EMB, HID), f32),
            pltpu.VMEM((HID, HID), f32),
            pltpu.SMEM((LOCAL_STRUCTS,), jnp.int32),
            pltpu.SemaphoreType.DMA((3,)),
        ],
        compiler_params=granted(12),
    )(
        *(
            pltpu.with_memory_space_constraint(operand, pltpu.HBM)
            for operand in (
                tagged_atom[None],
                observed_in[None],
                observed_in,
                positions,
                neighbours,
                atom_species[None],
                embed_scale,
                embed_shift,
                first_weight,
                first_bias[None],
                middle_weight,
                middle_bias[None],
                energy_weight,
                targets[None],
                noise_level[None],
            )
        )
    )
    partner = mine + lax.ppermute(theirs, "block_2", [(0, 1), (1, 0)])
    across_y = jnp.sum(exchanged(partner, "block_1"), axis=0)
    across_z = jnp.sum(exchanged(across_y, "block_0"), axis=0)
    gathered = exchanged(jnp.broadcast_to(across_z[None], (GROUPS, 8, OBS_DP * HID)), DP)
    columns, sent = pl.pallas_call(
        product_kernel,
        out_shape=(
            jax.ShapeDtypeStruct((OBS, ORDER), f32),
            jax.ShapeDtypeStruct((GROUPS, OBS + 8, ROWS), f32),
        ),
        in_specs=[VMEM] * 3,
        out_specs=(VMEM, VMEM),
        compiler_params=granted(8),
    )(gathered, covariance, predicted)
    products = exchanged(sent, DP)
    grams = pl.pallas_call(
        gram_kernel,
        out_shape=jax.ShapeDtypeStruct((8, OBS // 2, LANES), f32),
        in_specs=[VMEM] * 2,
        out_specs=VMEM,
        scratch_shapes=[pltpu.VMEM((OBS, ORDER), f32)],
        compiler_params=granted(8),
    )(columns, products)
    near = pl.pallas_call(
        summed_kernel,
        out_shape=jax.ShapeDtypeStruct((4, OBS // 2, LANES), f32),
        in_specs=[VMEM],
        out_specs=VMEM,
        compiler_params=granted(4),
    )(exchanged(grams, ("block_1", "block_2")))
    return pl.pallas_call(
        update_kernel,
        out_shape=(
            jax.ShapeDtypeStruct((1, ROWS), f32),
            jax.ShapeDtypeStruct((1, ROWS, ORDER), f32),
        ),
        in_specs=[VMEM] * 5,
        out_specs=(VMEM, HBM),
        scratch_shapes=[
            pltpu.VMEM((3 * OBS, ORDER), jnp.bfloat16),
            pltpu.VMEM((ROWS, ORDER), f32),
            pltpu.SemaphoreType.DMA((4,)),
        ],
        compiler_params=granted(12),
    )(
        exchanged(near, "block_0"),
        products,
        sent,
        covariance,
        kept,
    )


def solution(mesh):
    finer = Mesh(
        mesh.devices.reshape(4, 4, 4, 4, 2), ("dp_0", "dp_1", "block_0", "block_1", "block_2")
    )
    placed = (
        P(None, DP_BLOCK),
        P(None, DP_BLOCK),
        P(DP_BLOCK),
        P(DP_BLOCK),
        P(DP_BLOCK),
        P(),
        P(),
        P(),
        P(),
        P(),
        P(),
        P(),
        P(),
        P(),
        P(BLOCK, DP, None),
    )
    weighting = OBS / (LOCAL_STRUCTS * mesh.devices.size)
    return jax.shard_map(
        functools.partial(local, weighting=weighting),
        mesh=finer,
        in_specs=placed,
        out_specs=(P(BLOCK, DP), P(BLOCK, DP, None)),
        check_vma=False,
    )
```

```python
import functools

import jax
import jax.numpy as jnp
from jax import lax
from jax.experimental import pallas as pl
from jax.experimental.pallas import tpu as pltpu
from jax.sharding import Mesh
from jax.sharding import PartitionSpec as P

OBS = 64
GROUPS = 16
OBS_DP = 4
STRUCT = 32
LOCAL_STRUCTS = 8
ATOMS = 256
LANES = 128
HID = 256
EMB = 128
SLOTS = 16
ORDER = 2048
ROWS = 128
DP = ("dp_0", "dp_1")
BLOCK = ("block_0", "block_1", "block_2")
DP_BLOCK = ("dp_0", "dp_1", "block_0", "block_1", "block_2")

radial_width = 4.0
forgetting = 0.98
highest = lax.Precision.HIGHEST

VMEM = pl.BlockSpec(memory_space=pltpu.VMEM)
SMEM = pl.BlockSpec(memory_space=pltpu.SMEM)
HBM = pl.BlockSpec(memory_space=pltpu.HBM)


def granted(mib):
    return pltpu.CompilerParams(vmem_limit_bytes=mib * 1024 * 1024)


def contract(lhs, rhs, over):
    return lax.dot_general(
        lhs, rhs, ((over[:1], over[1:]), ((), ())), precision=highest, preferred_element_type=jnp.float32
    )


def halves(values):
    upper = values.astype(jnp.bfloat16)
    return upper, (values - upper.astype(jnp.float32)).astype(jnp.bfloat16)


def stacked(values, order):
    pair = halves(values)
    return jnp.concatenate([pair[n] for n in order], axis=0)


def plain(lhs, rhs, over):
    return lax.dot_general(
        lhs, rhs, ((over[:1], over[1:]), ((), ())), preferred_element_type=jnp.float32
    )


def along_lanes(row, at):
    return jnp.take_along_axis(
        jnp.broadcast_to(row, at.shape), at, axis=1, mode="promise_in_bounds"
    )


def jacobian_kernel(
    tags,
    parts,
    observed_source,
    positions,
    neighbours,
    species,
    scale,
    shift,
    first_source,
    first_bias,
    middle_source,
    middle_bias,
    energy_weight,
    targets,
    noise,
    mine,
    theirs,
    predicted,
    kept,
    tables,
    descriptor,
    features,
    jacobian,
    first_weight,
    middle_weight,
    observed,
    arrivals,
    weighting,
):
    core = lax.axis_index("block_2")
    block, group = lax.axis_index(BLOCK), lax.axis_index(DP)
    observed_copy = pltpu.make_async_copy(observed_source, observed, arrivals.at[2])
    observed_copy.start()
    first_copy = pltpu.make_async_copy(first_source, first_weight, arrivals.at[0])
    middle_copy = pltpu.make_async_copy(middle_source, middle_weight, arrivals.at[1])
    first_copy.start()
    middle_copy.start()
    for kind, table in enumerate((scale, shift)):
        columns = table[:].T
        for s in range(4):
            tables[kind * 4 + s] = jnp.broadcast_to(columns[:, s : s + 1], (EMB, LANES))
    lane = lax.broadcasted_iota(jnp.int32, (SLOTS, LANES), 1)
    for half in range(2):
        lanes = slice(half * LANES, (half + 1) * LANES)
        tag = jnp.zeros((SLOTS, LANES), jnp.int32)
        part = jnp.zeros((SLOTS, LANES), jnp.int32)
        for s in range(4):
            here = lane // STRUCT == s
            own = slice(half * 4 + s, half * 4 + s + 1)
            tag = jnp.where(here, tags[:, own], tag)
            part = jnp.where(here, parts[:, own], part)
        listed = neighbours[:, lanes]
        within = jnp.minimum(listed, STRUCT - 1)
        at = lane // STRUCT * STRUCT + within
        distance_sq = jnp.zeros((SLOTS, LANES), jnp.float32)
        chosen = jnp.zeros((SLOTS, LANES), jnp.float32)
        for c in range(3):
            row = positions[c : c + 1, lanes]
            displace = along_lanes(row, at) - row
            distance_sq = distance_sq + displace * displace
            chosen = jnp.where(part == c + 1, displace, chosen)
        radial = jnp.exp(-distance_sq / radial_width) * (listed < STRUCT).astype(jnp.float32)
        moved = (within == tag).astype(jnp.float32) - (lane % STRUCT == tag).astype(jnp.float32)
        radial_dot = radial * (-2.0 / radial_width) * chosen * moved
        near = along_lanes(species[:, lanes], at)
        odd = (near & 1) == 1
        upper = near >= 2

        def embed(step, carry, half=half, radial=radial, radial_dot=radial_dot, odd=odd, upper=upper):
            start = pl.multiple_of(step * 16, 16)
            rows = pl.ds(start, 16)
            held = [tables[n, rows, :] for n in range(8)]
            total = jnp.zeros((16, LANES), jnp.float32)
            tangent = jnp.zeros((16, LANES), jnp.float32)
            for k in range(SLOTS):
                r = jnp.broadcast_to(radial[k : k + 1], (16, LANES))
                r_dot = jnp.broadcast_to(radial_dot[k : k + 1], (16, LANES))
                is_odd = jnp.broadcast_to(odd[k : k + 1], (16, LANES))
                is_upper = jnp.broadcast_to(upper[k : k + 1], (16, LANES))
                slope = jnp.where(
                    is_upper,
                    jnp.where(is_odd, held[3], held[2]),
                    jnp.where(is_odd, held[1], held[0]),
                )
                offset = jnp.where(
                    is_upper,
                    jnp.where(is_odd, held[7], held[6]),
                    jnp.where(is_odd, held[5], held[4]),
                )
                steep = r * slope
                bent = jnp.tanh(steep + offset)
                total = total + r * bent
                tangent = tangent + r_dot * (bent + steep * (1.0 - bent * bent))
            descriptor[rows, half * LANES : (half + 1) * LANES] = total / SLOTS
            descriptor[rows, ATOMS + half * LANES : ATOMS + (half + 1) * LANES] = tangent / SLOTS
            return carry

        lax.fori_loop(0, EMB // 16, embed, 0)

    first_copy.wait()
    inner = plain(
        stacked(descriptor[:], (0, 1, 0)), stacked(first_weight[:], (0, 0, 1)), (0, 0)
    )
    first = jnp.tanh(inner[:ATOMS] + first_bias[:])
    upper, lower = halves(
        jnp.concatenate([first, (1.0 - first * first) * inner[ATOMS:]], axis=0)
    )
    for s in range(LOCAL_STRUCTS):
        for n, piece in enumerate((upper, upper, lower, lower)):
            source = n % 2 * ATOMS + s * STRUCT
            start = (s * 4 + n) * STRUCT
            features[start : start + STRUCT] = piece[source : source + STRUCT]
    middle_copy.wait()
    wide, narrow = halves(middle_weight[:])
    outer = (plain(upper, narrow, (1, 0)) + plain(lower, wide, (1, 0))) + plain(
        upper, wide, (1, 0)
    )
    second = jnp.tanh(outer[:ATOMS] + middle_bias[:])
    bend = 1.0 - second * second
    second_dot = bend * outer[ATOMS:]
    own = lax.broadcasted_iota(jnp.int32, (4, ATOMS), 0) == species[:]
    readout = contract(own.astype(jnp.float32), energy_weight[:], (0, 0))
    slope = readout * bend
    slope_dot = -2.0 * readout * second * second_dot
    energy = readout * second
    force = -(readout * second_dot)
    turned = features[:].T
    observed_copy.wait()
    jacobian[:] = jnp.zeros((OBS_DP, HID, HID), jnp.float32)
    sums = [jnp.zeros((1, HID), jnp.float32) for _ in range(OBS_DP)]
    for s in range(LOCAL_STRUCTS):
        rows = slice(s * STRUCT, (s + 1) * STRUCT)
        q = observed[s]
        is_energy = q == 0
        head, tail = halves(
            jnp.concatenate(
                [
                    jnp.where(
                        is_energy, slope[rows] * (weighting / STRUCT), slope_dot[rows] * -weighting
                    ),
                    slope[rows] * -weighting,
                ],
                axis=0,
            )
        )
        value = jnp.sum(
            jnp.where(is_energy, energy[rows] * (weighting / STRUCT), force[rows] * weighting),
            axis=0,
            keepdims=True,
        )
        for o in range(OBS_DP):
            sums[o] = sums[o] + jnp.where(q == o, value, 0.0)
        lanes = turned[:, s * 4 * STRUCT : (s + 1) * 4 * STRUCT]
        jacobian[q] += plain(
            jnp.concatenate([lanes, lanes], axis=1),
            jnp.concatenate([head, head, tail, jnp.zeros_like(tail)], axis=0),
            (1, 0),
        )
    predicted[:] = jnp.zeros((8, LANES), jnp.float32)
    for o in range(OBS_DP):
        predicted[o : o + 1, :] = sums[o][:, :LANES] + sums[o][:, LANES:]
    for y in range(4):
        for z in range(4):
            pair = (z * 8 + y * 2) * 8
            ours = pl.multiple_of(pair + core * 8, 8)
            other = pl.multiple_of(pair + (1 - core) * 8, 8)
            for q in range(OBS_DP):
                columns = slice(q * HID, (q + 1) * HID)
                mine[y, z, :, columns] = jacobian[q, pl.ds(ours, 8), :]
                theirs[y, z, :, columns] = jacobian[q, pl.ds(other, 8), :]
    line = middle_weight[pl.ds(block * 8 + group // 2, 1), :]
    kept[0:1] = jnp.where(group % 2 == 0, line[:, :LANES], line[:, LANES:])
    kept[1:2] = jnp.concatenate([targets[:], noise[:]], axis=1)
    kept[2:8] = jnp.zeros((6, LANES), jnp.float32)


def product_kernel(gathered, covariance, predicted, columns, sent):
    for i in range(8):
        for q in range(OBS_DP):
            for z in range(4):
                start = q * GROUPS + z * 4
                columns[start : start + 4, i * HID : (i + 1) * HID] = gathered[
                    :, z, i, q * HID : (q + 1) * HID
                ]
    product = contract(columns[:], covariance[0], (1, 1))
    for d in range(GROUPS):
        sent[d, :OBS] = product
        sent[d, OBS:] = predicted[:]


def gram_kernel(columns, products, sent, wide):
    for d in range(GROUPS):
        wide[:, d * ROWS : (d + 1) * ROWS] = products[d, :OBS]
    gram = contract(columns[:], wide[:], (1, 1))
    half = OBS // 2
    values = jnp.sum(
        jnp.concatenate([products[:, OBS + q, :] for q in range(OBS_DP)], axis=0),
        axis=1,
        keepdims=True,
    )
    packed = jnp.concatenate(
        [
            gram[:half],
            gram[half:, half:],
            values[:half],
            values[half:],
            jnp.zeros((half, half - 2), jnp.float32),
        ],
        axis=1,
    )
    for k in range(8):
        sent[k] = packed


def summed_kernel(arrived, sent):
    total = arrived[0]
    for k in range(1, 8):
        total = total + arrived[k]
    for k in range(4):
        sent[k] = total


def update_kernel(
    arrived,
    products,
    sent,
    covariance,
    kept,
    new_weights,
    new_covariance,
    wide,
    result,
    departures,
):
    half = OBS // 2
    packed = (arrived[0] + arrived[1]) + (arrived[2] + arrived[3])
    gram = jnp.concatenate(
        [
            jnp.concatenate([packed[:, :half], 2.0 * packed[:, half:OBS]], axis=1),
            jnp.concatenate(
                [jnp.zeros((half, half), jnp.float32), packed[:, OBS : OBS + half]], axis=1
            ),
        ],
        axis=0,
    )
    gram = 0.5 * (gram + gram.T)
    observed = jnp.concatenate([packed[:, 96:97], packed[:, 97:98]], axis=0)
    down = lax.broadcasted_iota(jnp.int32, (OBS, OBS), 0)
    across = lax.broadcasted_iota(jnp.int32, (OBS, OBS), 1)
    source = across == down % GROUPS * OBS_DP + down // GROUPS
    noise_here = jnp.sum(jnp.where(source, kept[1:2, OBS:], 0.0), axis=1, keepdims=True)
    target_here = jnp.sum(jnp.where(source, kept[1:2, :OBS], 0.0), axis=1, keepdims=True)
    identity = (down == across).astype(jnp.float32)
    gram = gram + jnp.where(down == across, noise_here, 0.0)
    work = jnp.concatenate([gram, identity], axis=1)
    strips = [work[8 * k : 8 * k + 8] for k in range(8)]
    sublane = lax.broadcasted_iota(jnp.int32, (8, LANES), 0)
    roots = []
    for k in range(0, 8, 2):
        active = range(k, 8)
        panel = [
            {r: jnp.broadcast_to(strips[r][:, 8 * k + j : 8 * k + j + 1], (8, LANES)) for r in active}
            for j in range(16)
        ]
        pivots = {k: jnp.ones((8, LANES), jnp.float32), k + 1: jnp.ones((8, LANES), jnp.float32)}
        for j in range(0, 16, 2):
            c, i = k + j // 8, j % 8
            left, right = panel[j], panel[j + 1]
            live = range(c, 8)
            top = jnp.broadcast_to(left[c][i : i + 1], (8, LANES))
            side = jnp.broadcast_to(right[c][i : i + 1], (8, LANES))
            corner = jnp.broadcast_to(right[c][i + 1 : i + 2], (8, LANES))
            area = top * corner - side * side
            inverse = 1.0 / area
            one = {r: (left[r] * corner - right[r] * side) * inverse for r in live}
            two = {r: (right[r] * top - left[r] * side) * inverse for r in live}
            one[c] = jnp.where(sublane > i + 1, one[c], 0.0)
            two[c] = jnp.where(sublane > i + 1, two[c], 0.0)
            for n in range(j + 2, 16):
                head = jnp.broadcast_to(panel[n][c][i : i + 1], (8, LANES))
                tail = jnp.broadcast_to(panel[n][c][i + 1 : i + 2], (8, LANES))
                for r in live:
                    panel[n][r] = panel[n][r] - (one[r] * head + two[r] * tail)
            head = jnp.broadcast_to(strips[c][i : i + 1], (8, LANES))
            tail = jnp.broadcast_to(strips[c][i + 1 : i + 2], (8, LANES))
            for r in live:
                strips[r] = strips[r] - (one[r] * head + two[r] * tail)
            ratio = 1.0 / top
            strips[c] = jnp.where(sublane == i + 1, strips[c] - side * ratio * head, strips[c])
            pivots[c] = jnp.where(sublane == i, top, pivots[c])
            pivots[c] = jnp.where(sublane == i + 1, area * ratio, pivots[c])
        for c in (k, k + 1):
            roots.append(strips[c] * lax.rsqrt(pivots[c]))
    root = jnp.concatenate(roots, axis=0)[:, OBS:]
    for d in range(GROUPS):
        wide[:, d * ROWS : (d + 1) * ROWS] = stacked(products[d, :OBS], (0, 0, 1))
    own = sent[0, :OBS]
    gain = contract(root, contract(root, own, (1, 0)), (0, 0))
    new_weights[:] = kept[0:1] + jnp.sum(gain * (target_here - observed), axis=0, keepdims=True)
    turned = stacked(gain, (0, 1, 0))
    copies = []
    for c in range(4):
        columns = slice(c * ORDER // 4, (c + 1) * ORDER // 4)
        update = plain(turned, wide[:, columns], (0, 0))
        result[:, columns] = (covariance[0, :, columns] - update) / forgetting
        copy = pltpu.make_async_copy(
            result.at[:, columns], new_covariance.at[0, :, columns], departures.at[c]
        )
        copy.start()
        copies.append(copy)
    for copy in copies:
        copy.wait()


def exchanged(tiles, axes):
    return lax.all_to_all(tiles, axes, split_axis=0, concat_axis=0, tiled=True)


def local(
    positions,
    neighbours,
    atom_species,
    tagged_atom,
    observed_in,
    targets,
    noise_level,
    embed_scale,
    embed_shift,
    first_weight,
    first_bias,
    middle_weight,
    middle_bias,
    energy_weight,
    covariance,
    weighting,
):
    f32 = jnp.float32
    mine, theirs, predicted, kept = pl.pallas_call(
        functools.partial(jacobian_kernel, weighting=weighting),
        out_shape=(
            jax.ShapeDtypeStruct((4, 4, 8, OBS_DP * HID), f32),
            jax.ShapeDtypeStruct((4, 4, 8, OBS_DP * HID), f32),
            jax.ShapeDtypeStruct((8, LANES), f32),
            jax.ShapeDtypeStruct((8, LANES), f32),
        ),
        in_specs=[VMEM, VMEM, HBM] + [VMEM] * 5 + [HBM, VMEM, HBM] + [VMEM] * 4,
        out_specs=(VMEM, VMEM, VMEM, VMEM),
        scratch_shapes=[
            pltpu.VMEM((8, EMB, LANES), f32),
            pltpu.VMEM((EMB, 2 * ATOMS), f32),
            pltpu.VMEM((4 * ATOMS, HID), jnp.bfloat16),
            pltpu.VMEM((OBS_DP, HID, HID), f32),
            pltpu.VMEM((EMB, HID), f32),
            pltpu.VMEM((HID, HID), f32),
            pltpu.SMEM((LOCAL_STRUCTS,), jnp.int32),
            pltpu.SemaphoreType.DMA((3,)),
        ],
        compiler_params=granted(12),
    )(
        *(
            pltpu.with_memory_space_constraint(operand, pltpu.HBM)
            for operand in (
                tagged_atom[None],
                observed_in[None],
                observed_in,
                positions,
                neighbours,
                atom_species[None],
                embed_scale,
                embed_shift,
                first_weight,
                first_bias[None],
                middle_weight,
                middle_bias[None],
                energy_weight,
                targets[None],
                noise_level[None],
            )
        )
    )
    partner = mine + lax.ppermute(theirs, "block_2", [(0, 1), (1, 0)])
    across_y = jnp.sum(exchanged(partner, "block_1"), axis=0)
    across_z = jnp.sum(exchanged(across_y, "block_0"), axis=0)
    along_z = exchanged(jnp.broadcast_to(across_z[None], (4, 8, OBS_DP * HID)), "dp_0")
    gathered = exchanged(jnp.broadcast_to(along_z[None], (4, 4, 8, OBS_DP * HID)), "dp_1")
    columns, sent = pl.pallas_call(
        product_kernel,
        out_shape=(
            jax.ShapeDtypeStruct((OBS, ORDER), f32),
            jax.ShapeDtypeStruct((GROUPS, OBS + 8, ROWS), f32),
        ),
        in_specs=[VMEM] * 3,
        out_specs=(VMEM, VMEM),
        compiler_params=granted(8),
    )(gathered, covariance, predicted)
    products = exchanged(sent, DP)
    grams = pl.pallas_call(
        gram_kernel,
        out_shape=jax.ShapeDtypeStruct((8, OBS // 2, LANES), f32),
        in_specs=[VMEM] * 2,
        out_specs=VMEM,
        scratch_shapes=[pltpu.VMEM((OBS, ORDER), f32)],
        compiler_params=granted(8),
    )(columns, products)
    near = pl.pallas_call(
        summed_kernel,
        out_shape=jax.ShapeDtypeStruct((4, OBS // 2, LANES), f32),
        in_specs=[VMEM],
        out_specs=VMEM,
        compiler_params=granted(4),
    )(exchanged(grams, ("block_1", "block_2")))
    return pl.pallas_call(
        update_kernel,
        out_shape=(
            jax.ShapeDtypeStruct((1, ROWS), f32),
            jax.ShapeDtypeStruct((1, ROWS, ORDER), f32),
        ),
        in_specs=[VMEM] * 5,
        out_specs=(VMEM, HBM),
        scratch_shapes=[
            pltpu.VMEM((3 * OBS, ORDER), jnp.bfloat16),
            pltpu.VMEM((ROWS, ORDER), f32),
            pltpu.SemaphoreType.DMA((4,)),
        ],
        compiler_params=granted(12),
    )(
        exchanged(near, "block_0"),
        products,
        sent,
        covariance,
        kept,
    )


def solution(mesh):
    finer = Mesh(
        mesh.devices.reshape(4, 4, 4, 4, 2), ("dp_0", "dp_1", "block_0", "block_1", "block_2")
    )
    placed = (
        P(None, DP_BLOCK),
        P(None, DP_BLOCK),
        P(DP_BLOCK),
        P(DP_BLOCK),
        P(DP_BLOCK),
        P(),
        P(),
        P(),
        P(),
        P(),
        P(),
        P(),
        P(),
        P(),
        P(BLOCK, DP, None),
    )
    weighting = OBS / (LOCAL_STRUCTS * mesh.devices.size)
    return jax.shard_map(
        functools.partial(local, weighting=weighting),
        mesh=finer,
        in_specs=placed,
        out_specs=(P(BLOCK, DP), P(BLOCK, DP, None)),
        check_vma=False,
    )
```

```python
import functools

import jax
import jax.numpy as jnp
from jax import lax
from jax.experimental import pallas as pl
from jax.experimental.pallas import tpu as pltpu
from jax.sharding import Mesh
from jax.sharding import PartitionSpec as P

OBS = 64
GROUPS = 16
OBS_DP = 4
STRUCT = 32
LOCAL_STRUCTS = 8
ATOMS = 256
LANES = 128
HID = 256
EMB = 128
SLOTS = 16
ORDER = 2048
ROWS = 128
DP = ("dp_0", "dp_1")
BLOCK = ("block_0", "block_1", "block_2")
DP_BLOCK = ("dp_0", "dp_1", "block_0", "block_1", "block_2")

radial_width = 4.0
forgetting = 0.98
highest = lax.Precision.HIGHEST

VMEM = pl.BlockSpec(memory_space=pltpu.VMEM)
SMEM = pl.BlockSpec(memory_space=pltpu.SMEM)
HBM = pl.BlockSpec(memory_space=pltpu.HBM)


def granted(mib):
    return pltpu.CompilerParams(vmem_limit_bytes=mib * 1024 * 1024)


def contract(lhs, rhs, over):
    return lax.dot_general(
        lhs, rhs, ((over[:1], over[1:]), ((), ())), precision=highest, preferred_element_type=jnp.float32
    )


def halves(values):
    upper = values.astype(jnp.bfloat16)
    return upper, (values - upper.astype(jnp.float32)).astype(jnp.bfloat16)


def stacked(values, order):
    pair = halves(values)
    return jnp.concatenate([pair[n] for n in order], axis=0)


def plain(lhs, rhs, over):
    return lax.dot_general(
        lhs, rhs, ((over[:1], over[1:]), ((), ())), preferred_element_type=jnp.float32
    )


def along_lanes(row, at):
    return jnp.take_along_axis(
        jnp.broadcast_to(row, at.shape), at, axis=1, mode="promise_in_bounds"
    )


def jacobian_kernel(
    tags,
    parts,
    observed_source,
    positions,
    neighbours,
    species,
    scale,
    shift,
    first_source,
    first_bias,
    middle_source,
    middle_bias,
    energy_weight,
    targets,
    noise,
    mine,
    theirs,
    predicted,
    kept,
    tables,
    descriptor,
    features,
    jacobian,
    first_weight,
    middle_weight,
    observed,
    arrivals,
    weighting,
):
    core = lax.axis_index("block_2")
    block, group = lax.axis_index(BLOCK), lax.axis_index(DP)
    observed_copy = pltpu.make_async_copy(observed_source, observed, arrivals.at[2])
    observed_copy.start()
    first_copy = pltpu.make_async_copy(first_source, first_weight, arrivals.at[0])
    middle_copy = pltpu.make_async_copy(middle_source, middle_weight, arrivals.at[1])
    first_copy.start()
    middle_copy.start()
    for kind, table in enumerate((scale, shift)):
        columns = table[:].T
        for s in range(4):
            tables[kind * 4 + s] = jnp.broadcast_to(columns[:, s : s + 1], (EMB, LANES))
    lane = lax.broadcasted_iota(jnp.int32, (SLOTS, LANES), 1)
    for half in range(2):
        lanes = slice(half * LANES, (half + 1) * LANES)
        tag = jnp.zeros((SLOTS, LANES), jnp.int32)
        part = jnp.zeros((SLOTS, LANES), jnp.int32)
        for s in range(4):
            here = lane // STRUCT == s
            own = slice(half * 4 + s, half * 4 + s + 1)
            tag = jnp.where(here, tags[:, own], tag)
            part = jnp.where(here, parts[:, own], part)
        listed = neighbours[:, lanes]
        within = jnp.minimum(listed, STRUCT - 1)
        at = lane // STRUCT * STRUCT + within
        distance_sq = jnp.zeros((SLOTS, LANES), jnp.float32)
        chosen = jnp.zeros((SLOTS, LANES), jnp.float32)
        for c in range(3):
            row = positions[c : c + 1, lanes]
            displace = along_lanes(row, at) - row
            distance_sq = distance_sq + displace * displace
            chosen = jnp.where(part == c + 1, displace, chosen)
        radial = jnp.exp(-distance_sq / radial_width) * (listed < STRUCT).astype(jnp.float32)
        moved = (within == tag).astype(jnp.float32) - (lane % STRUCT == tag).astype(jnp.float32)
        radial_dot = radial * (-2.0 / radial_width) * chosen * moved
        near = along_lanes(species[:, lanes], at)
        odd = (near & 1) == 1
        upper = near >= 2

        def embed(step, carry, half=half, radial=radial, radial_dot=radial_dot, odd=odd, upper=upper):
            start = pl.multiple_of(step * 16, 16)
            rows = pl.ds(start, 16)
            held = [tables[n, rows, :] for n in range(8)]
            total = jnp.zeros((16, LANES), jnp.float32)
            tangent = jnp.zeros((16, LANES), jnp.float32)
            for k in range(SLOTS):
                r = jnp.broadcast_to(radial[k : k + 1], (16, LANES))
                r_dot = jnp.broadcast_to(radial_dot[k : k + 1], (16, LANES))
                is_odd = jnp.broadcast_to(odd[k : k + 1], (16, LANES))
                is_upper = jnp.broadcast_to(upper[k : k + 1], (16, LANES))
                slope = jnp.where(
                    is_upper,
                    jnp.where(is_odd, held[3], held[2]),
                    jnp.where(is_odd, held[1], held[0]),
                )
                offset = jnp.where(
                    is_upper,
                    jnp.where(is_odd, held[7], held[6]),
                    jnp.where(is_odd, held[5], held[4]),
                )
                steep = r * slope
                bent = jnp.tanh(steep + offset)
                total = total + r * bent
                tangent = tangent + r_dot * (bent + steep * (1.0 - bent * bent))
            descriptor[rows, half * LANES : (half + 1) * LANES] = total / SLOTS
            descriptor[rows, ATOMS + half * LANES : ATOMS + (half + 1) * LANES] = tangent / SLOTS
            return carry

        lax.fori_loop(0, EMB // 16, embed, 0)

    first_copy.wait()
    inner = plain(
        stacked(descriptor[:], (0, 1, 0)), stacked(first_weight[:], (0, 0, 1)), (0, 0)
    )
    first = jnp.tanh(inner[:ATOMS] + first_bias[:])
    upper, lower = halves(
        jnp.concatenate([first, (1.0 - first * first) * inner[ATOMS:]], axis=0)
    )
    for s in range(LOCAL_STRUCTS):
        for n, piece in enumerate((upper, upper, lower, lower)):
            source = n % 2 * ATOMS + s * STRUCT
            start = (s * 4 + n) * STRUCT
            features[start : start + STRUCT] = piece[source : source + STRUCT]
    middle_copy.wait()
    wide, narrow = halves(middle_weight[:])
    outer = (plain(upper, narrow, (1, 0)) + plain(lower, wide, (1, 0))) + plain(
        upper, wide, (1, 0)
    )
    second = jnp.tanh(outer[:ATOMS] + middle_bias[:])
    bend = 1.0 - second * second
    second_dot = bend * outer[ATOMS:]
    own = lax.broadcasted_iota(jnp.int32, (4, ATOMS), 0) == species[:]
    chosen_species = own.astype(jnp.float32).astype(jnp.bfloat16)
    coarse, rest = energy_weight[:].astype(jnp.bfloat16), energy_weight[:]
    rest = rest - coarse.astype(jnp.float32)
    middle, fine = halves(rest)
    readout = plain(chosen_species, coarse, (0, 0)) + (
        plain(chosen_species, middle, (0, 0)) + plain(chosen_species, fine, (0, 0))
    )
    slope = readout * bend
    slope_dot = -2.0 * readout * second * second_dot
    energy = readout * second
    force = -(readout * second_dot)
    turned = features[:].T
    observed_copy.wait()
    jacobian[:] = jnp.zeros((OBS_DP, HID, HID), jnp.float32)
    sums = [jnp.zeros((1, HID), jnp.float32) for _ in range(OBS_DP)]
    for s in range(LOCAL_STRUCTS):
        rows = slice(s * STRUCT, (s + 1) * STRUCT)
        q = observed[s]
        is_energy = q == 0
        head, tail = halves(
            jnp.concatenate(
                [
                    jnp.where(
                        is_energy, slope[rows] * (weighting / STRUCT), slope_dot[rows] * -weighting
                    ),
                    slope[rows] * -weighting,
                ],
                axis=0,
            )
        )
        value = jnp.sum(
            jnp.where(is_energy, energy[rows] * (weighting / STRUCT), force[rows] * weighting),
            axis=0,
            keepdims=True,
        )
        for o in range(OBS_DP):
            sums[o] = sums[o] + jnp.where(q == o, value, 0.0)
        lanes = turned[:, s * 4 * STRUCT : (s + 1) * 4 * STRUCT]
        jacobian[q] += plain(
            jnp.concatenate([lanes, lanes], axis=1),
            jnp.concatenate([head, head, tail, jnp.zeros_like(tail)], axis=0),
            (1, 0),
        )
    predicted[:] = jnp.zeros((8, LANES), jnp.float32)
    for o in range(OBS_DP):
        predicted[o : o + 1, :] = sums[o][:, :LANES] + sums[o][:, LANES:]
    for y in range(4):
        for z in range(4):
            pair = (z * 8 + y * 2) * 8
            ours = pl.multiple_of(pair + core * 8, 8)
            other = pl.multiple_of(pair + (1 - core) * 8, 8)
            for q in range(OBS_DP):
                columns = slice(q * HID, (q + 1) * HID)
                mine[y, z, :, columns] = jacobian[q, pl.ds(ours, 8), :]
                theirs[y, z, :, columns] = jacobian[q, pl.ds(other, 8), :]
    line = middle_weight[pl.ds(block * 8 + group // 2, 1), :]
    kept[0:1] = jnp.where(group % 2 == 0, line[:, :LANES], line[:, LANES:])
    kept[1:2] = jnp.concatenate([targets[:], noise[:]], axis=1)
    kept[2:8] = jnp.zeros((6, LANES), jnp.float32)


def product_kernel(gathered, covariance, predicted, columns, sent):
    for i in range(8):
        for q in range(OBS_DP):
            for z in range(4):
                start = q * GROUPS + z * 4
                columns[start : start + 4, i * HID : (i + 1) * HID] = gathered[
                    :, z, i, q * HID : (q + 1) * HID
                ]
    product = contract(columns[:], covariance[0], (1, 1))
    for d in range(GROUPS):
        sent[d, :OBS] = product
        sent[d, OBS:] = predicted[:]


def gram_kernel(columns, products, sent, wide):
    for d in range(GROUPS):
        wide[:, d * ROWS : (d + 1) * ROWS] = products[d, :OBS]
    gram = contract(columns[:], wide[:], (1, 1))
    half = OBS // 2
    values = jnp.sum(
        jnp.concatenate([products[:, OBS + q, :] for q in range(OBS_DP)], axis=0),
        axis=1,
        keepdims=True,
    )
    packed = jnp.concatenate(
        [
            gram[:half],
            gram[half:, half:],
            values[:half],
            values[half:],
            jnp.zeros((half, half - 2), jnp.float32),
        ],
        axis=1,
    )
    for k in range(8):
        sent[k] = packed


def summed_kernel(arrived, sent):
    total = arrived[0]
    for k in range(1, 8):
        total = total + arrived[k]
    for k in range(4):
        sent[k] = total


def update_kernel(
    arrived,
    products,
    sent,
    covariance,
    kept,
    new_weights,
    new_covariance,
    wide,
    result,
    departures,
):
    half = OBS // 2
    packed = (arrived[0] + arrived[1]) + (arrived[2] + arrived[3])
    gram = jnp.concatenate(
        [
            jnp.concatenate([packed[:, :half], 2.0 * packed[:, half:OBS]], axis=1),
            jnp.concatenate(
                [jnp.zeros((half, half), jnp.float32), packed[:, OBS : OBS + half]], axis=1
            ),
        ],
        axis=0,
    )
    gram = 0.5 * (gram + gram.T)
    observed = jnp.concatenate([packed[:, 96:97], packed[:, 97:98]], axis=0)
    down = lax.broadcasted_iota(jnp.int32, (OBS, OBS), 0)
    across = lax.broadcasted_iota(jnp.int32, (OBS, OBS), 1)
    source = across == down % GROUPS * OBS_DP + down // GROUPS
    noise_here = jnp.sum(jnp.where(source, kept[1:2, OBS:], 0.0), axis=1, keepdims=True)
    target_here = jnp.sum(jnp.where(source, kept[1:2, :OBS], 0.0), axis=1, keepdims=True)
    identity = (down == across).astype(jnp.float32)
    gram = gram + jnp.where(down == across, noise_here, 0.0)
    work = jnp.concatenate([gram, identity], axis=1)
    strips = [work[8 * k : 8 * k + 8] for k in range(8)]
    sublane = lax.broadcasted_iota(jnp.int32, (8, LANES), 0)
    roots = []
    for k in range(0, 8, 2):
        active = range(k, 8)
        panel = [
            {r: jnp.broadcast_to(strips[r][:, 8 * k + j : 8 * k + j + 1], (8, LANES)) for r in active}
            for j in range(16)
        ]
        pivots = {k: jnp.ones((8, LANES), jnp.float32), k + 1: jnp.ones((8, LANES), jnp.float32)}
        for j in range(0, 16, 2):
            c, i = k + j // 8, j % 8
            left, right = panel[j], panel[j + 1]
            live = range(c, 8)
            top = jnp.broadcast_to(left[c][i : i + 1], (8, LANES))
            side = jnp.broadcast_to(right[c][i : i + 1], (8, LANES))
            corner = jnp.broadcast_to(right[c][i + 1 : i + 2], (8, LANES))
            area = top * corner - side * side
            inverse = 1.0 / area
            one = {r: (left[r] * corner - right[r] * side) * inverse for r in live}
            two = {r: (right[r] * top - left[r] * side) * inverse for r in live}
            one[c] = jnp.where(sublane > i + 1, one[c], 0.0)
            two[c] = jnp.where(sublane > i + 1, two[c], 0.0)
            for n in range(j + 2, 16):
                head = jnp.broadcast_to(panel[n][c][i : i + 1], (8, LANES))
                tail = jnp.broadcast_to(panel[n][c][i + 1 : i + 2], (8, LANES))
                for r in live:
                    panel[n][r] = panel[n][r] - (one[r] * head + two[r] * tail)
            head = jnp.broadcast_to(strips[c][i : i + 1], (8, LANES))
            tail = jnp.broadcast_to(strips[c][i + 1 : i + 2], (8, LANES))
            for r in live:
                strips[r] = strips[r] - (one[r] * head + two[r] * tail)
            ratio = 1.0 / top
            strips[c] = jnp.where(sublane == i + 1, strips[c] - side * ratio * head, strips[c])
            pivots[c] = jnp.where(sublane == i, top, pivots[c])
            pivots[c] = jnp.where(sublane == i + 1, area * ratio, pivots[c])
        for c in (k, k + 1):
            roots.append(strips[c] * lax.rsqrt(pivots[c]))
    root = jnp.concatenate(roots, axis=0)[:, OBS:]
    for d in range(GROUPS):
        wide[:, d * ROWS : (d + 1) * ROWS] = stacked(products[d, :OBS], (0, 0, 1))
    own = sent[0, :OBS]
    gain = contract(root, contract(root, own, (1, 0)), (0, 0))
    new_weights[:] = kept[0:1] + jnp.sum(gain * (target_here - observed), axis=0, keepdims=True)
    turned = stacked(gain, (0, 1, 0))
    copies = []
    for c in range(4):
        columns = slice(c * ORDER // 4, (c + 1) * ORDER // 4)
        update = plain(turned, wide[:, columns], (0, 0))
        result[:, columns] = (covariance[0, :, columns] - update) / forgetting
        copy = pltpu.make_async_copy(
            result.at[:, columns], new_covariance.at[0, :, columns], departures.at[c]
        )
        copy.start()
        copies.append(copy)
    for copy in copies:
        copy.wait()


def exchanged(tiles, axes):
    return lax.all_to_all(tiles, axes, split_axis=0, concat_axis=0, tiled=True)


def local(
    positions,
    neighbours,
    atom_species,
    tagged_atom,
    observed_in,
    targets,
    noise_level,
    embed_scale,
    embed_shift,
    first_weight,
    first_bias,
    middle_weight,
    middle_bias,
    energy_weight,
    covariance,
    weighting,
):
    f32 = jnp.float32
    mine, theirs, predicted, kept = pl.pallas_call(
        functools.partial(jacobian_kernel, weighting=weighting),
        out_shape=(
            jax.ShapeDtypeStruct((4, 4, 8, OBS_DP * HID), f32),
            jax.ShapeDtypeStruct((4, 4, 8, OBS_DP * HID), f32),
            jax.ShapeDtypeStruct((8, LANES), f32),
            jax.ShapeDtypeStruct((8, LANES), f32),
        ),
        in_specs=[VMEM, VMEM, HBM] + [VMEM] * 5 + [HBM, VMEM, HBM] + [VMEM] * 4,
        out_specs=(VMEM, VMEM, VMEM, VMEM),
        scratch_shapes=[
            pltpu.VMEM((8, EMB, LANES), f32),
            pltpu.VMEM((EMB, 2 * ATOMS), f32),
            pltpu.VMEM((4 * ATOMS, HID), jnp.bfloat16),
            pltpu.VMEM((OBS_DP, HID, HID), f32),
            pltpu.VMEM((EMB, HID), f32),
            pltpu.VMEM((HID, HID), f32),
            pltpu.SMEM((LOCAL_STRUCTS,), jnp.int32),
            pltpu.SemaphoreType.DMA((3,)),
        ],
        compiler_params=granted(12),
    )(
        *(
            pltpu.with_memory_space_constraint(operand, pltpu.HBM)
            for operand in (
                tagged_atom[None],
                observed_in[None],
                observed_in,
                positions,
                neighbours,
                atom_species[None],
                embed_scale,
                embed_shift,
                first_weight,
                first_bias[None],
                middle_weight,
                middle_bias[None],
                energy_weight,
                targets[None],
                noise_level[None],
            )
        )
    )
    partner = mine + lax.ppermute(theirs, "block_2", [(0, 1), (1, 0)])
    across_y = jnp.sum(exchanged(partner, "block_1"), axis=0)
    across_z = jnp.sum(exchanged(across_y, "block_0"), axis=0)
    along_z = exchanged(jnp.broadcast_to(across_z[None], (4, 8, OBS_DP * HID)), "dp_0")
    gathered = exchanged(jnp.broadcast_to(along_z[None], (4, 4, 8, OBS_DP * HID)), "dp_1")
    columns, sent = pl.pallas_call(
        product_kernel,
        out_shape=(
            jax.ShapeDtypeStruct((OBS, ORDER), f32),
            jax.ShapeDtypeStruct((GROUPS, OBS + 8, ROWS), f32),
        ),
        in_specs=[VMEM] * 3,
        out_specs=(VMEM, VMEM),
        compiler_params=granted(8),
    )(gathered, covariance, predicted)
    products = exchanged(sent, DP)
    grams = pl.pallas_call(
        gram_kernel,
        out_shape=jax.ShapeDtypeStruct((8, OBS // 2, LANES), f32),
        in_specs=[VMEM] * 2,
        out_specs=VMEM,
        scratch_shapes=[pltpu.VMEM((OBS, ORDER), f32)],
        compiler_params=granted(8),
    )(columns, products)
    near = pl.pallas_call(
        summed_kernel,
        out_shape=jax.ShapeDtypeStruct((4, OBS // 2, LANES), f32),
        in_specs=[VMEM],
        out_specs=VMEM,
        compiler_params=granted(4),
    )(exchanged(grams, ("block_1", "block_2")))
    return pl.pallas_call(
        update_kernel,
        out_shape=(
            jax.ShapeDtypeStruct((1, ROWS), f32),
            jax.ShapeDtypeStruct((1, ROWS, ORDER), f32),
        ),
        in_specs=[VMEM] * 5,
        out_specs=(VMEM, HBM),
        scratch_shapes=[
            pltpu.VMEM((3 * OBS, ORDER), jnp.bfloat16),
            pltpu.VMEM((ROWS, ORDER), f32),
            pltpu.SemaphoreType.DMA((4,)),
        ],
        compiler_params=granted(12),
    )(
        exchanged(near, "block_0"),
        products,
        sent,
        covariance,
        kept,
    )


def solution(mesh):
    finer = Mesh(
        mesh.devices.reshape(4, 4, 4, 4, 2), ("dp_0", "dp_1", "block_0", "block_1", "block_2")
    )
    placed = (
        P(None, DP_BLOCK),
        P(None, DP_BLOCK),
        P(DP_BLOCK),
        P(DP_BLOCK),
        P(DP_BLOCK),
        P(),
        P(),
        P(),
        P(),
        P(),
        P(),
        P(),
        P(),
        P(),
        P(BLOCK, DP, None),
    )
    weighting = OBS / (LOCAL_STRUCTS * mesh.devices.size)
    return jax.shard_map(
        functools.partial(local, weighting=weighting),
        mesh=finer,
        in_specs=placed,
        out_specs=(P(BLOCK, DP), P(BLOCK, DP, None)),
        check_vma=False,
    )
```
